128 devices in a mesh: sx: 16 (over x, y_lo, core), sy: 8 (over z, y_hi).
Axes of the slice: x: 4, y: 4 (y_hi: 2, y_lo: 2; y = y_hi * 2 + y_lo), z: 4, core: 2. Of those that a mesh axis runs over, the one named last changes fastest.
Arguments:
- queries: bfloat16 [8192, 128, 128], P(('sx', 'sy')), may hold values from -8 to 8
- keys: bfloat16 [8192, 8, 128], P(('sx', 'sy')), may hold values from -8 to 8
- values: bfloat16 [8192, 8, 128], P(('sx', 'sy')), may hold values from -6 to 6
Outputs:
- attention: bfloat16 [8192, 128, 128], P(('sx', 'sy'))
The draws below stay inside these ranges and needn't reach their ends.
All inputs are finite; a program needn't handle non-finite values.
Results may differ from the reference program's by a relative error of at most 0.005.
Values may be sent and summed in bfloat16 or wider, within the bound.
No kernel may reach another device: no remote copies, remote signals or barrier semaphores. Data moves between devices by JAX's collectives and lax.ppermute only.
A program may use at most 64 MiB of HBM per device.

```python
import math
import jax
import jax.numpy as jnp
from jax import lax

HEAD_DIM = 128
HEADS = 128
KV_HEADS = 8
TOKENS = 8192


def shard_levels(own_key, dims, shards, low, high):
    loudness = 1.0
    for axis_at, shards_of in shards:
        heights = jax.random.uniform(jax.random.fold_in(jax.random.fold_in(own_key, 6), axis_at), (shards_of,), jnp.float32, low / len(shards), high / len(shards))
        loudness = loudness * jnp.repeat(jnp.exp(heights), dims[axis_at] // shards_of).reshape((-1,) + (1,) * (len(dims) - 1 - axis_at))
    return loudness


def noise(key, shape, width, most, cuts=(), kind=jnp.bfloat16):
    entries = jax.random.normal(key, shape, jnp.float32) * width
    if len(cuts) > 0:
        entries = shard_levels(key, shape, cuts, -0.22, 0.18) * entries
    return jnp.clip(entries, min=-most, max=most).astype(kind)


def setup_inputs(seed: int = 0) -> dict:
    key_of = jax.random.split(jax.random.key(seed), 4)
    return {
        "queries": noise(key_of[0], (TOKENS, HEADS, HEAD_DIM), 1.6, 8.0, ((0, 128),)),
        "keys": noise(key_of[1], (TOKENS, KV_HEADS, HEAD_DIM), 1.6, 8.0, ((0, 128),)),
        "values": noise(key_of[2], (TOKENS, KV_HEADS, HEAD_DIM), 1.0, 6.0, ((0, 128),)),
    }


def frequencies(head_width):
    half_index = jnp.arange(head_width // 2, dtype=jnp.float32)
    base_rate = jnp.power(jnp.float32(500000.0), -2.0 * half_index / head_width)
    wavelen = 2.0 * math.pi / base_rate
    smooth = (8192.0 / wavelen - 1.0) / 3.0
    blended = (1.0 - smooth) * base_rate / 8.0 + smooth * base_rate
    return jnp.where(wavelen < 2048.0, base_rate, jnp.where(wavelen > 8192.0, base_rate / 8.0, blended))

def rotate(heads_in, positions):
    head_width = heads_in.shape[-1]
    half_width = head_width // 2
    angles = positions.astype(jnp.float32)[:, None] * frequencies(head_width)[None, :]
    cosine = jnp.cos(angles)[:, None, :]
    sine_wave = jnp.sin(angles)[:, None, :]
    widened = heads_in.astype(jnp.float32)
    front = widened[..., :half_width]
    second = widened[..., half_width:]
    turned = jnp.concatenate([front * cosine - second * sine_wave, second * cosine + front * sine_wave], axis=-1)
    return turned.astype(jnp.bfloat16)

def reference(queries, keys, values):
    total_rows, heads_all, head_width = queries.shape
    group_size = heads_all // keys.shape[1]
    positions = jnp.arange(total_rows, dtype=jnp.int32)
    query_rot = lax.optimization_barrier(rotate(queries, positions))
    key_rot = lax.optimization_barrier(rotate(keys, positions))
    score_scale = 1.0 / math.sqrt(head_width)
    block_size = total_rows // 8

    def one_head(head_index):
        query_head = lax.dynamic_index_in_dim(query_rot, head_index, 1, keepdims=False)
        key_index = (head_index // group_size).astype(jnp.int32)
        key_head = lax.dynamic_index_in_dim(key_rot, key_index, 1, keepdims=False)
        value_head = lax.dynamic_index_in_dim(values, key_index, 1, keepdims=False)
        pieces = []
        for block_index in range(8):
            row_begin = block_index * block_size
            key_end = row_begin + block_size
            query_rows = query_head[row_begin:key_end]
            scores = jnp.dot(query_rows, key_head[:key_end].T, preferred_element_type=jnp.float32) * score_scale
            allowed = positions[:key_end][None, :] <= positions[row_begin:key_end][:, None]
            scores = jnp.where(allowed, scores, -jnp.inf)
            weights = jnp.exp(scores - lax.optimization_barrier(jnp.max(scores, axis=1, keepdims=True)))
            summed = jnp.dot(weights.astype(jnp.bfloat16), value_head[:key_end], preferred_element_type=jnp.float32)
            pieces.append(summed / lax.optimization_barrier(jnp.sum(weights, axis=1, keepdims=True)))
        return jnp.concatenate(pieces, axis=0).astype(jnp.bfloat16)
    result = lax.map(one_head, jnp.arange(heads_all, dtype=jnp.int32))
    return jnp.transpose(result, (1, 0, 2))
```

```python
import math

import jax
import jax.numpy as jnp
from jax import lax
from jax.experimental import pallas as pl
from jax.experimental.pallas import tpu as pltpu
from jax.sharding import PartitionSpec as P

LOG2E = 1.4426950408889634
SAFE = 110.0
CHUNKS = 2
TILE = 512


def frequencies(head_width):
    half_index = jnp.arange(head_width // 2, dtype=jnp.float32)
    base_rate = jnp.power(jnp.float32(500000.0), -2.0 * half_index / head_width)
    wavelen = 2.0 * math.pi / base_rate
    smooth = (8192.0 / wavelen - 1.0) / 3.0
    blended = (1.0 - smooth) * base_rate / 8.0 + smooth * base_rate
    return jnp.where(
        wavelen < 2048.0, base_rate, jnp.where(wavelen > 8192.0, base_rate / 8.0, blended)
    )


def rotate(heads_in, positions):
    head_width = heads_in.shape[-1]
    half_width = head_width // 2
    angles = positions.astype(jnp.float32)[:, None] * frequencies(head_width)[None, :]
    cosine = jnp.cos(angles)[:, None, :]
    sine_wave = jnp.sin(angles)[:, None, :]
    widened = heads_in.astype(jnp.float32)
    front = widened[..., :half_width]
    second = widened[..., half_width:]
    turned = jnp.concatenate(
        [front * cosine - second * sine_wave, second * cosine + front * sine_wave], axis=-1
    )
    return turned.astype(jnp.bfloat16)


def attn(q, kv, ksq, *, bq, strip, period, offset, sub=256, unroll=2):
    R, D = q.shape
    NB = kv.shape[0]
    BK = kv.shape[1] // 2
    c = LOG2E / math.sqrt(D)
    span = bq // strip * period
    nd = max(span // BK, 1)
    nsub = BK // sub

    def kernel(ksq_ref, q_ref, kv_ref, o_ref, qT_ref):
        qi = pl.program_id(0)
        pos0 = qi * span
        n_full = pos0 // BK
        qT_ref[...] = q_ref[...].astype(jnp.float32).T.astype(jnp.bfloat16)
        qf = q_ref[...].astype(jnp.float32)
        qsq = jnp.max(jnp.sum(qf * qf, axis=1))
        lane = lax.broadcasted_iota(jnp.int32, (1, bq), 1)
        qpos = pos0 + offset + lane // strip * period + lane % strip

        def block(blk, carry, masked):
            acc, l = carry
            for s in range(nsub):
                k = kv_ref[blk, s * sub:(s + 1) * sub, :]
                st = lax.dot_general(k, qT_ref[...], (((1,), (0,)), ((), ())), preferred_element_type=jnp.float32)
                p = jnp.exp2(st * c)
                if masked:
                    kpos = blk * BK + s * sub + lax.broadcasted_iota(jnp.int32, (sub, 1), 0)
                    p = jnp.where(kpos <= qpos, p, 0.0)
                l = l + jnp.sum(p.reshape(sub // 8, 8, bq), axis=0)
                vT = jnp.concatenate([kv_ref[blk, BK + s * sub + t * 128: BK + s * sub + (t + 1) * 128, :] for t in range(sub // 128)], axis=1)
                acc = acc + lax.dot_general(vT, p.astype(jnp.bfloat16), (((1,), (0,)), ((), ())), preferred_element_type=jnp.float32)
            return acc, l

        def finish(acc, l):
            o = acc / jnp.sum(l, axis=0, keepdims=True)
            o_ref[...] = o.T.astype(jnp.bfloat16)

        carry = (jnp.zeros((D, bq), jnp.float32), jnp.zeros((8, bq), jnp.float32))
        def body(j, cr):
            for u in range(unroll):
                cr = block(j * unroll + u, cr, False)
            return cr
        n_main = n_full // unroll
        carry = lax.fori_loop(0, n_main, body, carry)
        if unroll > 1:
            carry = lax.fori_loop(n_main * unroll, n_full, lambda j, cr: block(j, cr, False), carry)
        for t in range(nd):
            carry = block(n_full + t, carry, True)
        finish(*carry)

        @pl.when(jnp.logical_not(qsq * ksq_ref[0, 0] * (c * c) < SAFE * SAFE))
        def _():
            def slow(blk, cr):
                acc, l, m = cr
                for s in range(nsub):
                    k = kv_ref[blk, s * sub:(s + 1) * sub, :]
                    st = lax.dot_general(k, qT_ref[...], (((1,), (0,)), ((), ())), preferred_element_type=jnp.float32) * c
                    kpos = blk * BK + s * sub + lax.broadcasted_iota(jnp.int32, (sub, 1), 0)
                    st = jnp.where(kpos <= qpos, st, -jnp.inf)
                    mn = jnp.maximum(m, jnp.max(st, axis=0, keepdims=True))
                    a = jnp.exp2(m - mn)
                    p = jnp.exp2(st - mn)
                    l = l * a + jnp.sum(p, axis=0, keepdims=True)
                    vT = jnp.concatenate([kv_ref[blk, BK + s * sub + t * 128: BK + s * sub + (t + 1) * 128, :] for t in range(sub // 128)], axis=1)
                    acc = acc * a + lax.dot_general(vT, p.astype(jnp.bfloat16), (((1,), (0,)), ((), ())), preferred_element_type=jnp.float32)
                    m = mn
                return acc, l, m
            acc, l, m = lax.fori_loop(0, n_full + nd, slow, (jnp.zeros((D, bq), jnp.float32), jnp.zeros((1, bq), jnp.float32), jnp.full((1, bq), -1e30, jnp.float32)))
            o_ref[...] = (acc / l).T.astype(jnp.bfloat16)

    return pl.pallas_call(
        kernel, grid=(R // bq,),
        in_specs=[pl.BlockSpec(memory_space=pltpu.SMEM),
                  pl.BlockSpec((bq, D), lambda i: (i, 0)),
                  pl.BlockSpec(kv.shape, lambda i: (0, 0, 0))],
        out_specs=pl.BlockSpec((bq, D), lambda i: (i, 0)),
        out_shape=jax.ShapeDtypeStruct((R, D), jnp.bfloat16),
        scratch_shapes=[pltpu.VMEM((D, bq), jnp.bfloat16)],
        compiler_params=pltpu.CompilerParams(vmem_limit_bytes=40 * 2**20),
        name="attn",
    )(ksq, q, kv)


def shards(queries, keys, values):
    rows, heads_all, width = queries.shape
    key_heads = keys.shape[1]
    group = heads_all // key_heads
    start_row = lax.axis_index(("sx", "sy")) * rows
    positions = start_row + jnp.arange(rows, dtype=jnp.int32)
    strip = rows // CHUNKS
    everyone = ("sx", "sy")

    key_rot = rotate(keys, positions)
    pair = jnp.stack([key_rot, values], axis=1)
    pair = lax.all_to_all(pair, "sy", split_axis=2, concat_axis=0, tiled=True)[:, :, 0]
    own_keys, own_values = pair[:, 0], pair[:, 1]
    block = own_keys.shape[0]
    own_values = own_values.reshape(block // 128, 128, width).swapaxes(1, 2).reshape(block, width)
    kv = lax.all_gather(jnp.concatenate([own_keys, own_values], axis=0), "sx", axis=0)
    wide = kv[:, :block].astype(jnp.float32)
    ksq = jnp.max(jnp.sum(wide * wide, axis=-1)).reshape(1, 1)

    query_rot = rotate(queries, positions)
    ordered = (
        query_rot.reshape(rows, key_heads, group, width)
        .transpose(0, 2, 1, 3)
        .reshape(rows, heads_all, width)
    )
    arrived = []
    for c in range(CHUNKS):
        piece = ordered[c * strip:(c + 1) * strip]
        arrived.append(lax.all_to_all(piece, everyone, split_axis=1, concat_axis=0, tiled=True)[:, 0])
    back = []
    for c in range(CHUNKS):
        done = attn(arrived[c], kv, ksq, bq=TILE, strip=strip, period=rows, offset=c * strip,
                    sub=256, unroll=2)
        done = done.reshape(heads_all, strip, width).swapaxes(0, 1)
        back.append(lax.all_to_all(done, everyone, split_axis=1, concat_axis=1, tiled=True))
    merged = jnp.concatenate(back, axis=0)
    return (
        merged.reshape(rows, group, key_heads, width)
        .transpose(0, 2, 1, 3)
        .reshape(rows, heads_all, width)
    )


def solution(mesh):
    placed = (P(("sx", "sy"), None, None),) * 3
    return jax.shard_map(
        shards, mesh=mesh, in_specs=placed, out_specs=P(("sx", "sy"), None, None), check_vma=False
    )
```

```python
import math

import jax
import jax.numpy as jnp
from jax import lax
from jax.experimental import pallas as pl
from jax.experimental.pallas import tpu as pltpu
from jax.sharding import Mesh, PartitionSpec as P

LOG2E = 1.4426950408889634
LOW, HIGH = 2.0**-80, 2.0**100
CHUNKS = 2
TILE = 2048
AXES = ("x", "yl", "core", "sy")


def frequencies(head_width):
    half_index = jnp.arange(head_width // 2, dtype=jnp.float32)
    base_rate = jnp.power(jnp.float32(500000.0), -2.0 * half_index / head_width)
    wavelen = 2.0 * math.pi / base_rate
    smooth = (8192.0 / wavelen - 1.0) / 3.0
    blended = (1.0 - smooth) * base_rate / 8.0 + smooth * base_rate
    return jnp.where(
        wavelen < 2048.0, base_rate, jnp.where(wavelen > 8192.0, base_rate / 8.0, blended)
    )


def rotate(heads_in, positions):
    head_width = heads_in.shape[-1]
    half_width = head_width // 2
    angles = positions.astype(jnp.float32)[:, None] * frequencies(head_width)[None, :]
    cosine = jnp.cos(angles)[:, None, :]
    sine_wave = jnp.sin(angles)[:, None, :]
    widened = heads_in.astype(jnp.float32)
    front = widened[..., :half_width]
    second = widened[..., half_width:]
    turned = jnp.concatenate(
        [front * cosine - second * sine_wave, second * cosine + front * sine_wave], axis=-1
    )
    return turned.astype(jnp.bfloat16)


def attn(q, pieces, where, *, bq, strip, period, which, sub=512, unroll=2):
    D = q.shape[-1]
    G = q.shape[0]
    BK = pieces[0].shape[1] // 2
    blocks = G * period // BK
    c = LOG2E / math.sqrt(D)
    devs = bq // strip
    nd = devs * period // BK
    w = bq // nd
    offset = which * strip

    def kernel(where_ref, q_ref, c_ref, cc_ref, u_ref, cu_ref, v_ref, cv_ref, h_ref, ch_ref, g_ref, cg_ref,
               o_ref, qT_ref, acc_ref, l_ref, kv_ref, sems):
        qi = pl.program_id(0)
        first = qi * nd

        @pl.when(qi == 0)
        def _():
            x, core = where_ref[0], where_ref[1]
            for step, refs in ((0, (c_ref, cc_ref)), (3, (u_ref, cu_ref)), (1, (v_ref, cv_ref)), (2, ((h_ref, g_ref), (ch_ref, cg_ref)))):
                for other in (0, 1):
                    for yl in (0, 1):
                        src = refs[other][yl].at[0] if step == 2 else refs[other].at[yl]
                        b = lax.rem(x + step, 4) * 4 + yl * 2 + lax.rem(core + other, 2)
                        pltpu.make_async_copy(src, kv_ref.at[b], sems.at[b]).start()

        for t in range(nd):
            pltpu.make_async_copy(c_ref.at[0], kv_ref.at[first + t], sems.at[first + t]).wait()

        qT_ref[...] = q_ref[...].reshape(bq, D).astype(jnp.float32).T.astype(jnp.bfloat16)

        def values(blk, lo, n):
            return jnp.concatenate(
                [kv_ref[blk, BK + lo + t * 128: BK + lo + (t + 1) * 128, :] for t in range(n // 128)], axis=1)

        def block(blk, lo, masked):
            for s in range(0, BK, sub):
                k = kv_ref[blk, s:s + sub, :]
                st = jnp.dot(k, qT_ref[:, lo:], preferred_element_type=jnp.float32)
                p = jnp.exp2(st * c)
                if masked:
                    lane = lax.broadcasted_iota(jnp.int32, (1, w), 1)
                    at = lane // strip * period + offset + lane % strip
                    row = s + lax.broadcasted_iota(jnp.int32, (sub, 1), 0)
                    head = jnp.where(row <= at, p[:, :w], 0.0)
                    p = jnp.concatenate([head, p[:, w:]], axis=1) if bq - lo > w else head
                l_ref[:, lo:] += jnp.sum(p.reshape(sub // 8, 8, bq - lo), axis=0)
                acc_ref[:, lo:] += jnp.dot(
                    values(blk, s, sub), p.astype(jnp.bfloat16), preferred_element_type=jnp.float32)

        acc_ref[...] = jnp.zeros_like(acc_ref)
        l_ref[...] = jnp.zeros_like(l_ref)

        def body(j, _):
            for u in range(unroll):
                block(j * unroll + u, 0, False)
            return 0

        lax.fori_loop(0, first // unroll, body, 0)
        for t in range(nd):
            block(first + t, t * w, True)
        total = jnp.sum(l_ref[...], axis=0, keepdims=True)
        o_ref[...] = (acc_ref[...] * (1.0 / total)).T.astype(jnp.bfloat16).reshape(o_ref.shape)
        fine = jnp.logical_and(jnp.min(total) > LOW, jnp.max(total) < HIGH)

        @pl.when(jnp.logical_not(fine))
        def _():
            lane = lax.broadcasted_iota(jnp.int32, (1, bq), 1)
            at = qi * devs * period + lane // strip * period + offset + lane % strip

            def slow(blk, state):
                l, m = state
                st = jnp.dot(kv_ref[blk, :BK, :], qT_ref[...], preferred_element_type=jnp.float32) * c
                row = blk * BK + lax.broadcasted_iota(jnp.int32, (BK, 1), 0)
                st = jnp.where(row <= at, st, -jnp.inf)
                top = jnp.maximum(m, jnp.max(st, axis=0, keepdims=True))
                shrink = jnp.exp2(m - top)
                p = jnp.exp2(st - top)
                acc_ref[...] = acc_ref[...] * shrink + jnp.dot(
                    values(blk, 0, BK), p.astype(jnp.bfloat16), preferred_element_type=jnp.float32)
                return l * shrink + jnp.sum(p, axis=0, keepdims=True), top

            acc_ref[...] = jnp.zeros_like(acc_ref)
            start = (jnp.zeros((1, bq), jnp.float32), jnp.full((1, bq), -1e30, jnp.float32))
            l, _ = lax.fori_loop(0, first + nd, slow, start)
            o_ref[...] = (acc_ref[...] / l).T.astype(jnp.bfloat16).reshape(o_ref.shape)

    anywhere = pl.BlockSpec(memory_space=pl.ANY)
    return pl.pallas_call(
        kernel, grid=(G // devs,),
        in_specs=[pl.BlockSpec(memory_space=pltpu.SMEM),
                  pl.BlockSpec((devs, strip, D), lambda i: (i, which, 0))] + [anywhere] * len(pieces),
        out_specs=pl.BlockSpec((devs, strip, D), lambda i: (i, 0, 0)),
        out_shape=jax.ShapeDtypeStruct((G, strip, D), jnp.bfloat16),
        scratch_shapes=[pltpu.VMEM((D, bq), jnp.bfloat16), pltpu.VMEM((D, bq), jnp.float32),
                        pltpu.VMEM((8, bq), jnp.float32), pltpu.VMEM((blocks, 2 * BK, D), jnp.bfloat16),
                        pltpu.SemaphoreType.DMA((blocks,))],
        compiler_params=pltpu.CompilerParams(vmem_limit_bytes=40 * 2**20),
        name="attn",
    )(where, q, *(pltpu.with_memory_space_constraint(piece, pltpu.HBM) for piece in pieces))


def shards(queries, keys, values):
    rows, heads_all, width = queries.shape
    key_heads = keys.shape[1]
    group = heads_all // key_heads
    x, yl, core, sy = (lax.axis_index(a) for a in AXES)
    start_row = lax.axis_index(AXES) * rows
    positions = start_row + jnp.arange(rows, dtype=jnp.int32)

    key_rot = rotate(keys, positions)
    pair = jnp.stack([key_rot, values], axis=1)
    pair = jnp.concatenate([pair, pair], axis=2)
    pair = lax.all_to_all(pair, ("yl", "sy"), split_axis=2, concat_axis=0, tiled=True)[:, :, 0]
    pair = pair.reshape(2, -1, 2, width)
    block = pair.shape[1]
    own_values = pair[:, :, 1].reshape(2, block // 128, 128, width).swapaxes(2, 3).reshape(2, block, width)
    c = jnp.concatenate([pair[:, :, 0], own_values], axis=1)
    ahead = [(i, (i + 1) % 4) for i in range(4)]
    behind = [(i, (i - 1) % 4) for i in range(4)]
    swap = [(0, 1), (1, 0)]
    u = lax.ppermute(c, "x", ahead)
    v = lax.ppermute(c, "x", behind)
    h = lax.ppermute(u[0:1], "x", ahead)
    g = lax.ppermute(v[1:2], "x", behind)
    pieces = []
    for piece in (c, u, v, h, g):
        pieces += [piece, lax.ppermute(piece, "core", swap)]
    where = jnp.stack([x, core]).astype(jnp.int32)

    query_rot = rotate(queries, positions)
    ordered = (
        query_rot.reshape(rows, key_heads, group, width)
        .transpose(0, 2, 1, 3)
        .reshape(rows, heads_all, width)
    )
    arrived = lax.all_to_all(ordered, AXES, split_axis=1, concat_axis=0, tiled=True)[:, 0]
    arrived = arrived.reshape(heads_all, rows, width)
    strip = rows // CHUNKS
    back = []
    for n in range(CHUNKS):
        done = attn(arrived, pieces, where, bq=TILE, strip=strip, period=rows, which=n)
        back.append(lax.all_to_all(done.swapaxes(0, 1), AXES, split_axis=1, concat_axis=1, tiled=True))
    merged = jnp.concatenate(back, axis=0)
    return (
        merged.reshape(rows, group, key_heads, width)
        .transpose(0, 2, 1, 3)
        .reshape(rows, heads_all, width)
    )


def solution(mesh):
    finer = Mesh(mesh.devices.reshape(4, 2, 2, 8), AXES)
    placed = P(AXES, None, None)
    return jax.shard_map(
        shards, mesh=finer, in_specs=(placed,) * 3, out_specs=placed, check_vma=False
    )
```

```python
import math

import jax
import jax.numpy as jnp
from jax import lax
from jax.experimental import pallas as pl
from jax.experimental.pallas import tpu as pltpu
from jax.sharding import Mesh, PartitionSpec as P


LOG2E = 1.4426950408889634
LOW, HIGH = 2.0**-80, 2.0**100
CHUNKS = 2
TILE = 2048
AXES = ("x", "yl", "core", "sy")


def frequencies(head_width):
    half_index = jnp.arange(head_width // 2, dtype=jnp.float32)
    base_rate = jnp.power(jnp.float32(500000.0), -2.0 * half_index / head_width)
    wavelen = 2.0 * math.pi / base_rate
    smooth = (8192.0 / wavelen - 1.0) / 3.0
    blended = (1.0 - smooth) * base_rate / 8.0 + smooth * base_rate
    return jnp.where(
        wavelen < 2048.0, base_rate, jnp.where(wavelen > 8192.0, base_rate / 8.0, blended)
    )


def rotate(heads_in, positions):
    head_width = heads_in.shape[-1]
    half_width = head_width // 2
    angles = positions.astype(jnp.float32)[:, None] * frequencies(head_width)[None, :]
    cosine = jnp.cos(angles)[:, None, :]
    sine_wave = jnp.sin(angles)[:, None, :]
    widened = heads_in.astype(jnp.float32)
    front = widened[..., :half_width]
    second = widened[..., half_width:]
    turned = jnp.concatenate(
        [front * cosine - second * sine_wave, second * cosine + front * sine_wave], axis=-1
    )
    return turned.astype(jnp.bfloat16)


def attn(q, pieces, where, out, *, bq, period, which, sub=512, unroll=2):
    G, strip, D = q.shape
    BK = pieces[0].shape[1] // 2
    blocks = G * period // BK
    c = LOG2E / math.sqrt(D)
    devs = bq // strip
    nd = devs * period // BK
    w = bq // nd
    offset = which * strip

    def kernel(where_ref, q_ref, c_ref, cc_ref, u_ref, cu_ref, v_ref, cv_ref, h_ref, ch_ref, g_ref, cg_ref,
               *rest):
        o_ref, qT_ref, acc_ref, l_ref, kv_ref, sems = rest[-6:]
        qi = pl.program_id(0)
        first = qi * nd

        @pl.when(qi == 0)
        def _():
            x, core = where_ref[0], where_ref[1]
            for step, refs in ((0, (c_ref, cc_ref)), (3, (u_ref, cu_ref)), (1, (v_ref, cv_ref)), (2, ((h_ref, g_ref), (ch_ref, cg_ref)))):
                for other in (0, 1):
                    for yl in (0, 1):
                        src = refs[other][yl].at[0] if step == 2 else refs[other].at[yl]
                        b = lax.rem(x + step, 4) * 4 + yl * 2 + lax.rem(core + other, 2)
                        pltpu.make_async_copy(src, kv_ref.at[b], sems.at[b]).start()

        for t in range(nd):
            pltpu.make_async_copy(c_ref.at[0], kv_ref.at[first + t], sems.at[first + t]).wait()

        qT_ref[...] = q_ref[...].reshape(bq, D).astype(jnp.float32).T.astype(jnp.bfloat16)

        def values(blk, lo, n):
            return jnp.concatenate(
                [kv_ref[blk, BK + lo + t * 128: BK + lo + (t + 1) * 128, :] for t in range(n // 128)], axis=1)

        def block(blk, lo, masked):
            for s in range(0, BK, sub):
                k = kv_ref[blk, s:s + sub, :]
                st = jnp.dot(k, qT_ref[:, lo:], preferred_element_type=jnp.float32)
                p = jnp.exp2(st * c)
                if masked:
                    lane = lax.broadcasted_iota(jnp.int32, (1, w), 1)
                    at = lane // strip * period + offset + lane % strip
                    row = s + lax.broadcasted_iota(jnp.int32, (sub, 1), 0)
                    head = jnp.where(row <= at, p[:, :w], 0.0)
                    p = jnp.concatenate([head, p[:, w:]], axis=1) if bq - lo > w else head
                l_ref[:, lo:] += jnp.sum(p.reshape(sub // 8, 8, bq - lo), axis=0)
                acc_ref[:, lo:] += jnp.dot(
                    values(blk, s, sub), p.astype(jnp.bfloat16), preferred_element_type=jnp.float32)

        acc_ref[...] = jnp.zeros_like(acc_ref)
        l_ref[...] = jnp.zeros_like(l_ref)

        def body(j, _):
            for u in range(unroll):
                block(j * unroll + u, 0, False)
            return 0

        lax.fori_loop(0, first // unroll, body, 0)
        for t in range(nd):
            block(first + t, t * w, True)
        total = jnp.sum(l_ref[...], axis=0, keepdims=True)
        o_ref[...] = (acc_ref[...] * (1.0 / total)).T.astype(jnp.bfloat16).reshape(o_ref.shape)
        fine = jnp.logical_and(jnp.min(total) > LOW, jnp.max(total) < HIGH)

        @pl.when(jnp.logical_not(fine))
        def _():
            lane = lax.broadcasted_iota(jnp.int32, (1, bq), 1)
            at = qi * devs * period + lane // strip * period + offset + lane % strip

            def slow(blk, state):
                l, m = state
                st = jnp.dot(kv_ref[blk, :BK, :], qT_ref[...], preferred_element_type=jnp.float32) * c
                row = blk * BK + lax.broadcasted_iota(jnp.int32, (BK, 1), 0)
                st = jnp.where(row <= at, st, -jnp.inf)
                top = jnp.maximum(m, jnp.max(st, axis=0, keepdims=True))
                shrink = jnp.exp2(m - top)
                p = jnp.exp2(st - top)
                acc_ref[...] = acc_ref[...] * shrink + jnp.dot(
                    values(blk, 0, BK), p.astype(jnp.bfloat16), preferred_element_type=jnp.float32)
                return l * shrink + jnp.sum(p, axis=0, keepdims=True), top

            acc_ref[...] = jnp.zeros_like(acc_ref)
            start = (jnp.zeros((1, bq), jnp.float32), jnp.full((1, bq), -1e30, jnp.float32))
            l, _ = lax.fori_loop(0, first + nd, slow, start)
            o_ref[...] = (acc_ref[...] / l).T.astype(jnp.bfloat16).reshape(o_ref.shape)

    extra = () if out is None else (out,)
    anywhere = pl.BlockSpec(memory_space=pl.ANY)
    return pl.pallas_call(
        kernel, grid=(G // devs,),
        in_specs=[pl.BlockSpec(memory_space=pltpu.SMEM),
                  pl.BlockSpec((devs, strip, D), lambda i: (i, 0, 0))] + [anywhere] * (len(pieces) + len(extra)),
        out_specs=pl.BlockSpec((devs, strip, D), lambda i: (i, which, 0)),
        out_shape=jax.ShapeDtypeStruct((G, period, D), jnp.bfloat16),
        input_output_aliases={2 + len(pieces): 0} if extra else {},
        scratch_shapes=[pltpu.VMEM((D, bq), jnp.bfloat16), pltpu.VMEM((D, bq), jnp.float32),
                        pltpu.VMEM((8, bq), jnp.float32), pltpu.VMEM((blocks, 2 * BK, D), jnp.bfloat16),
                        pltpu.SemaphoreType.DMA((blocks,))],
        compiler_params=pltpu.CompilerParams(vmem_limit_bytes=40 * 2**20),
        name="attn",
    )(where, q, *(pltpu.with_memory_space_constraint(piece, pltpu.HBM) for piece in pieces), *extra)


def shards(queries, keys, values):
    rows, heads_all, width = queries.shape
    key_heads = keys.shape[1]
    group = heads_all // key_heads
    x, _, core, _ = (lax.axis_index(a) for a in AXES)
    start_row = lax.axis_index(AXES) * rows
    positions = start_row + jnp.arange(rows, dtype=jnp.int32)

    key_rot = rotate(keys, positions)
    pair = jnp.stack([key_rot, values], axis=1)
    pair = jnp.concatenate([pair, pair], axis=2)
    pair = lax.all_to_all(pair, ("yl", "sy"), split_axis=2, concat_axis=0, tiled=True)[:, :, 0]
    pair = pair.reshape(2, -1, 2, width)
    block = pair.shape[1]
    own_values = pair[:, :, 1].reshape(2, block // 128, 128, width).swapaxes(2, 3).reshape(2, block, width)
    c = jnp.concatenate([pair[:, :, 0], own_values], axis=1)
    ahead = [(i, (i + 1) % 4) for i in range(4)]
    behind = [(i, (i - 1) % 4) for i in range(4)]
    swap = [(0, 1), (1, 0)]
    u = lax.ppermute(c, "x", ahead)
    v = lax.ppermute(c, "x", behind)
    h = lax.ppermute(u[0:1], "x", ahead)
    g = lax.ppermute(v[1:2], "x", behind)
    pieces = []
    for piece in (c, u, v, h, g):
        pieces += [piece, lax.ppermute(piece, "core", swap)]
    where = jnp.stack([x, core]).astype(jnp.int32)

    query_rot = rotate(queries, positions)
    ordered = (
        query_rot.reshape(rows, key_heads, group, width)
        .transpose(0, 2, 1, 3)
        .reshape(rows, heads_all, width)
    )
    strip = rows // CHUNKS
    arrived = []
    for n in range(CHUNKS):
        piece = lax.all_to_all(
            ordered[n * strip:(n + 1) * strip], AXES, split_axis=1, concat_axis=0, tiled=True)
        arrived.append(piece[:, 0].reshape(heads_all, strip, width))
    out = None
    for n in range(CHUNKS):
        out = attn(arrived[n], pieces, where, out, bq=TILE, period=rows, which=n)
    merged = lax.all_to_all(out.swapaxes(0, 1), AXES, split_axis=1, concat_axis=1, tiled=True)
    return (
        merged.reshape(rows, group, key_heads, width)
        .transpose(0, 2, 1, 3)
        .reshape(rows, heads_all, width)
    )


def solution(mesh):
    finer = Mesh(mesh.devices.reshape(4, 2, 2, 8), AXES)
    placed = P(AXES, None, None)

    return jax.shard_map(shards, mesh=finer, in_specs=(placed,) * 3, out_specs=placed, check_vma=False)
```

```python
import math

import jax
import jax.numpy as jnp
from jax import lax
from jax.experimental import pallas as pl
from jax.experimental.pallas import tpu as pltpu
from jax.sharding import Mesh, PartitionSpec as P


LOG2E = 1.4426950408889634
LOW, HIGH = 2.0**-80, 2.0**100
CHUNKS = 2
TILE = 2048
GROUPS = {8: {0: (0, 1), 1: tuple(range(2, 8))}}
AXES = ("x", "yl", "core", "sy")


def frequencies(head_width):
    half_index = jnp.arange(head_width // 2, dtype=jnp.float32)
    base_rate = jnp.power(jnp.float32(500000.0), -2.0 * half_index / head_width)
    wavelen = 2.0 * math.pi / base_rate
    smooth = (8192.0 / wavelen - 1.0) / 3.0
    blended = (1.0 - smooth) * base_rate / 8.0 + smooth * base_rate
    return jnp.where(
        wavelen < 2048.0, base_rate, jnp.where(wavelen > 8192.0, base_rate / 8.0, blended)
    )


def turned(head, cosine, signed_sine):
    return head * cosine + pltpu.roll(head, head.shape[-1] // 2, 1) * signed_sine


def prepare_pair(keys, values, cosine, signed_sine):
    rows, heads, width = keys.shape

    def kernel(k_ref, v_ref, cos_ref, sin_ref, o_ref, kf_ref, vf_ref):
        kf_ref[...] = k_ref[...].astype(jnp.float32)
        vf_ref[...] = v_ref[...].astype(jnp.float32)
        for h in range(heads):
            key = turned(kf_ref[:, h, :], cos_ref[...], sin_ref[...]).astype(jnp.bfloat16)
            value = vf_ref[:, h, :].astype(jnp.bfloat16)
            for half in (0, heads):
                o_ref[half + h, 0] = key
                o_ref[half + h, 1] = value

    wide = pltpu.VMEM((rows, heads, width), jnp.float32)
    return pl.pallas_call(
        kernel, out_shape=jax.ShapeDtypeStruct((2 * heads, 2, rows, width), jnp.bfloat16),
        scratch_shapes=[wide, wide], name="pair",
    )(keys, values, cosine, signed_sine)


def prepare_queries(queries, cosine, signed_sine, group):
    rows, heads, width = queries.shape
    strip = rows // CHUNKS

    def kernel(q_ref, cos_ref, sin_ref, *rest):
        outs, wide_ref = rest[:-1], rest[-1]
        wide_ref[...] = q_ref[...].astype(jnp.float32)
        for h in range(group):
            head = turned(wide_ref[:, h, :], cos_ref[...], sin_ref[...]).astype(jnp.bfloat16)
            for n, o_ref in enumerate(outs):
                o_ref[h, 0] = head[n * strip:(n + 1) * strip]

    table = pl.BlockSpec((rows, width), lambda g: (0, 0))
    parts = pl.pallas_call(
        kernel, grid=(heads // group,),
        in_specs=[pl.BlockSpec((rows, group, width), lambda g: (0, g, 0)), table, table],
        out_specs=[pl.BlockSpec((group, 1, strip, width), lambda g: (0, g, 0, 0))] * CHUNKS,
        out_shape=[jax.ShapeDtypeStruct((group, heads // group, strip, width), jnp.bfloat16)] * CHUNKS,
        scratch_shapes=[pltpu.VMEM((rows, group, width), jnp.float32)], name="queries",
    )(queries, cosine, signed_sine)
    return [part.reshape(heads, strip, width) for part in parts]


def attn(q, pieces, where, out, *, bq, period, which, sub=512, unroll=4):
    G, strip, D = q.shape
    BK = pieces[0].shape[1] // 2
    blocks = G * period // BK
    c = LOG2E / math.sqrt(D)
    devs = bq // strip
    nd = devs * period // BK
    w = bq // nd
    offset = which * strip
    groups = GROUPS[nd]

    def kernel(where_ref, q_ref, c_ref, cc_ref, u_ref, cu_ref, v_ref, cv_ref, h_ref, ch_ref, g_ref, cg_ref,
               *rest):
        o_ref, qT_ref, acc_ref, l_ref, kv_ref, qv_ref, sems = rest[-7:]
        qi = pl.program_id(0)
        first = qi * nd

        @pl.when(qi == 0)
        def _():
            pltpu.make_async_copy(q_ref, qv_ref, sems.at[blocks]).start()
            x, core = where_ref[0], where_ref[1]
            for step, refs in ((0, (c_ref, cc_ref)), (3, (u_ref, cu_ref)), (1, (v_ref, cv_ref)), (2, ((h_ref, g_ref), (ch_ref, cg_ref)))):
                for other in (0, 1):
                    for yl in (0, 1):
                        src = refs[other][yl].at[0] if step == 2 else refs[other].at[yl]
                        b = lax.rem(x + step, 4) * 4 + yl * 2 + lax.rem(core + other, 2)
                        pltpu.make_async_copy(src, kv_ref.at[b], sems.at[b]).start()

        @pl.when(qi == 0)
        def _():
            pltpu.make_async_copy(q_ref, qv_ref, sems.at[blocks]).wait()

        def landed(t):
            pltpu.make_async_copy(c_ref.at[0], kv_ref.at[first + t], sems.at[first + t]).wait()

        qT_ref[...] = qv_ref[pl.ds(qi * devs, devs)].reshape(bq, D).astype(jnp.float32).T.astype(jnp.bfloat16)

        def values(blk, lo, n):
            return jnp.concatenate(
                [kv_ref[blk, BK + lo + t * 128: BK + lo + (t + 1) * 128, :] for t in range(n // 128)], axis=1)

        def block(blk, lo, masked):
            for s in range(0, BK, sub):
                k = kv_ref[blk, s:s + sub, :]
                st = jnp.dot(k, qT_ref[:, lo:], preferred_element_type=jnp.float32)
                p = jnp.exp2(st * c)
                if masked:
                    lane = lax.broadcasted_iota(jnp.int32, (1, w), 1)
                    at = lane // strip * period + offset + lane % strip
                    row = s + lax.broadcasted_iota(jnp.int32, (sub, 1), 0)
                    head = jnp.where(row <= at, p[:, :w], 0.0)
                    p = jnp.concatenate([head, p[:, w:]], axis=1) if bq - lo > w else head
                l_ref[:, lo:] += jnp.sum(p.reshape(sub // 8, 8, bq - lo), axis=0)
                acc_ref[:, lo:] += jnp.dot(
                    values(blk, s, sub), p.astype(jnp.bfloat16), preferred_element_type=jnp.float32)

        acc_ref[...] = jnp.zeros_like(acc_ref)
        l_ref[...] = jnp.zeros_like(l_ref)

        def body(j, _):
            for u in range(unroll):
                block(j * unroll + u, 0, False)
            return 0

        lax.fori_loop(0, first // unroll, body, 0)
        for t in range(nd):
            for later in groups.get(t, ()):
                landed(later)
            block(first + t, t * w, True)
        total = jnp.sum(l_ref[...], axis=0, keepdims=True)
        o_ref[...] = (acc_ref[...] * (1.0 / total)).T.astype(jnp.bfloat16).reshape(o_ref.shape)
        fine = jnp.logical_and(jnp.min(total) > LOW, jnp.max(total) < HIGH)

        @pl.when(jnp.logical_not(fine))
        def _():
            lane = lax.broadcasted_iota(jnp.int32, (1, bq), 1)
            at = qi * devs * period + lane // strip * period + offset + lane % strip

            def slow(blk, state):
                l, m = state
                st = jnp.dot(kv_ref[blk, :BK, :], qT_ref[...], preferred_element_type=jnp.float32) * c
                row = blk * BK + lax.broadcasted_iota(jnp.int32, (BK, 1), 0)
                st = jnp.where(row <= at, st, -jnp.inf)
                top = jnp.maximum(m, jnp.max(st, axis=0, keepdims=True))
                shrink = jnp.exp2(m - top)
                p = jnp.exp2(st - top)
                acc_ref[...] = acc_ref[...] * shrink + jnp.dot(
                    values(blk, 0, BK), p.astype(jnp.bfloat16), preferred_element_type=jnp.float32)
                return l * shrink + jnp.sum(p, axis=0, keepdims=True), top

            acc_ref[...] = jnp.zeros_like(acc_ref)
            start = (jnp.zeros((1, bq), jnp.float32), jnp.full((1, bq), -1e30, jnp.float32))
            l, _ = lax.fori_loop(0, first + nd, slow, start)
            o_ref[...] = (acc_ref[...] / l).T.astype(jnp.bfloat16).reshape(o_ref.shape)

    extra = () if out is None else (out,)
    anywhere = pl.BlockSpec(memory_space=pl.ANY)
    return pl.pallas_call(
        kernel, grid=(G // devs,),
        in_specs=[pl.BlockSpec(memory_space=pltpu.SMEM),
                  anywhere] + [anywhere] * (len(pieces) + len(extra)),
        out_specs=pl.BlockSpec((devs, strip, D), lambda i: (i, which, 0)),
        out_shape=jax.ShapeDtypeStruct((G, period, D), jnp.bfloat16),
        input_output_aliases={2 + len(pieces): 0} if extra else {},
        scratch_shapes=[pltpu.VMEM((D, bq), jnp.bfloat16), pltpu.VMEM((D, bq), jnp.float32),
                        pltpu.VMEM((8, bq), jnp.float32), pltpu.VMEM((blocks, 2 * BK, D), jnp.bfloat16),
                        pltpu.VMEM((G, strip, D), jnp.bfloat16),
                        pltpu.SemaphoreType.DMA((blocks + 1,))],
        compiler_params=pltpu.CompilerParams(vmem_limit_bytes=24 * 2**20),
        name="attn",
    )(where, *(pltpu.with_memory_space_constraint(piece, pltpu.HBM) for piece in (q, *pieces)), *extra)


def shards(queries, keys, values):
    rows, heads_all, width = queries.shape
    key_heads = keys.shape[1]
    group = heads_all // key_heads
    x, _, core, _ = (lax.axis_index(a) for a in AXES)
    start_row = lax.axis_index(AXES) * rows
    positions = start_row + jnp.arange(rows, dtype=jnp.int32)

    angles = positions.astype(jnp.float32)[:, None] * jnp.tile(frequencies(width), 2)[None, :]
    cosine = jnp.cos(angles)
    signed_sine = jnp.sin(angles) * jnp.where(jnp.arange(width) < width // 2, -1.0, 1.0)

    pair = prepare_pair(keys, values, cosine, signed_sine)
    pair = lax.all_to_all(pair, ("yl", "sy"), split_axis=0, concat_axis=0, tiled=True)
    pair = pair.swapaxes(0, 1).reshape(2, 2, -1, width)
    block = pair.shape[2]
    own_values = pair[1].reshape(2, block // 128, 128, width).swapaxes(2, 3).reshape(2, block, width)
    c = jnp.concatenate([pair[0], own_values], axis=1)
    ahead = [(i, (i + 1) % 4) for i in range(4)]
    behind = [(i, (i - 1) % 4) for i in range(4)]
    swap = [(0, 1), (1, 0)]
    u = lax.ppermute(c, "x", ahead)
    v = lax.ppermute(c, "x", behind)
    h = lax.ppermute(u[0:1], "x", ahead)
    g = lax.ppermute(v[1:2], "x", behind)
    pieces = []
    for piece in (c, u, v, h, g):
        pieces += [piece, lax.ppermute(piece, "core", swap)]
    where = jnp.stack([x, core]).astype(jnp.int32)

    ordered = prepare_queries(queries, cosine, signed_sine, group)
    arrived = []
    for n in range(CHUNKS):
        arrived.append(lax.all_to_all(ordered[n], AXES, split_axis=0, concat_axis=0, tiled=True))
    out = None
    for n in range(CHUNKS):
        out = attn(arrived[n], pieces, where, out, bq=TILE, period=rows, which=n)
    merged = lax.all_to_all(out.swapaxes(0, 1), AXES, split_axis=1, concat_axis=1, tiled=True)
    return (
        merged.reshape(rows, group, key_heads, width)
        .transpose(0, 2, 1, 3)
        .reshape(rows, heads_all, width)
    )


def solution(mesh):
    finer = Mesh(mesh.devices.reshape(4, 2, 2, 8), AXES)
    placed = P(AXES, None, None)

    return jax.shard_map(shards, mesh=finer, in_specs=(placed,) * 3, out_specs=placed, check_vma=False)
```

```python
import math

import jax
import jax.numpy as jnp
from jax import lax
from jax.experimental import pallas as pl
from jax.experimental.pallas import tpu as pltpu
from jax.sharding import Mesh, PartitionSpec as P


LOG2E = 1.4426950408889634
LOW, HIGH = 2.0**-80, 2.0**100
CHUNKS = 2
TILE = 2048
GROUPS = {8: {0: (0,), 1: tuple(range(1, 8))}}
AXES = ("x", "yl", "core", "sy")


def frequencies(head_width):
    half_index = jnp.arange(head_width // 2, dtype=jnp.float32)
    base_rate = jnp.power(jnp.float32(500000.0), -2.0 * half_index / head_width)
    wavelen = 2.0 * math.pi / base_rate
    smooth = (8192.0 / wavelen - 1.0) / 3.0
    blended = (1.0 - smooth) * base_rate / 8.0 + smooth * base_rate
    return jnp.where(
        wavelen < 2048.0, base_rate, jnp.where(wavelen > 8192.0, base_rate / 8.0, blended)
    )


def turned(head, cosine, signed_sine):
    return head * cosine + pltpu.roll(head, head.shape[-1] // 2, 1) * signed_sine


def prepare_pair(keys, values, cosine, signed_sine):
    rows, heads, width = keys.shape

    def kernel(k_ref, v_ref, cos_ref, sin_ref, o_ref, kf_ref, vf_ref):
        kf_ref[...] = k_ref[...].astype(jnp.float32)
        vf_ref[...] = v_ref[...].astype(jnp.float32)
        for h in range(heads):
            key = turned(kf_ref[:, h, :], cos_ref[...], sin_ref[...]).astype(jnp.bfloat16)
            value = vf_ref[:, h, :].astype(jnp.bfloat16)
            for half in (0, heads):
                o_ref[half + h, 0] = key
                o_ref[half + h, 1] = value

    wide = pltpu.VMEM((rows, heads, width), jnp.float32)
    return pl.pallas_call(
        kernel, out_shape=jax.ShapeDtypeStruct((2 * heads, 2, rows, width), jnp.bfloat16),
        scratch_shapes=[wide, wide], name="pair",
    )(keys, values, cosine, signed_sine)


def prepare_queries(queries, cosine, signed_sine, group):
    rows, heads, width = queries.shape
    strip = rows // CHUNKS

    def kernel(q_ref, cos_ref, sin_ref, *rest):
        outs, wide_ref = rest[:-1], rest[-1]
        wide_ref[...] = q_ref[...].astype(jnp.float32)
        for h in range(group):
            head = turned(wide_ref[:, h, :], cos_ref[...], sin_ref[...]).astype(jnp.bfloat16)
            for n, o_ref in enumerate(outs):
                o_ref[h, 0] = head[n * strip:(n + 1) * strip]

    table = pl.BlockSpec((rows, width), lambda g: (0, 0))
    parts = pl.pallas_call(
        kernel, grid=(heads // group,),
        in_specs=[pl.BlockSpec((rows, group, width), lambda g: (0, g, 0)), table, table],
        out_specs=[pl.BlockSpec((group, 1, strip, width), lambda g: (0, g, 0, 0))] * CHUNKS,
        out_shape=[jax.ShapeDtypeStruct((group, heads // group, strip, width), jnp.bfloat16)] * CHUNKS,
        scratch_shapes=[pltpu.VMEM((rows, group, width), jnp.float32)], name="queries",
    )(queries, cosine, signed_sine)
    return [part.reshape(heads, strip, width) for part in parts]


def attn(q, pieces, where, out, *, bq, period, which, sub=512, unroll=4):
    G, strip, D = q.shape
    BK = pieces[0].shape[1] // 2
    blocks = G * period // BK
    c = LOG2E / math.sqrt(D)
    devs = bq // strip
    nd = devs * period // BK
    w = bq // nd
    offset = which * strip
    groups = GROUPS[nd]

    def kernel(where_ref, q_ref, c_ref, cc_ref, u_ref, cu_ref, v_ref, cv_ref, h_ref, ch_ref, g_ref, cg_ref,
               *rest):
        o_ref, qT_ref, acc_ref, l_ref, kv_ref, qv_ref, sems = rest[-7:]
        qi = pl.program_id(0)
        first = qi * nd

        @pl.when(qi == 0)
        def _():
            pltpu.make_async_copy(q_ref, qv_ref, sems.at[blocks]).start()
            x, core = where_ref[0], where_ref[1]
            for plane in range(4):
                for step, refs in ((0, (c_ref, cc_ref)), (3, (u_ref, cu_ref)), (1, (v_ref, cv_ref)),
                                   (2, ((h_ref, g_ref), (ch_ref, cg_ref)))):
                    @pl.when(lax.rem(x + step, 4) == plane)
                    def _():
                        for yl in (0, 1):
                            for other in (0, 1):
                                src = refs[other][yl].at[0] if step == 2 else refs[other].at[yl]
                                b = plane * 4 + yl * 2 + lax.rem(core + other, 2)
                                pltpu.make_async_copy(src, kv_ref.at[b], sems.at[b]).start()

        @pl.when(qi == 0)
        def _():
            pltpu.make_async_copy(q_ref, qv_ref, sems.at[blocks]).wait()

        def landed(t):
            pltpu.make_async_copy(c_ref.at[0], kv_ref.at[first + t], sems.at[first + t]).wait()


        def values(blk, lo, n):
            return jnp.concatenate(
                [kv_ref[blk, BK + lo + t * 128: BK + lo + (t + 1) * 128, :] for t in range(n // 128)], axis=1)

        def block(blk, lo, masked, fresh=False):
            for s in range(0, BK, sub):
                k = kv_ref[blk, s:s + sub, :]
                rows = qv_ref[pl.ds(qi * devs + lo // strip, devs - lo // strip)].reshape(bq - lo, D)
                st = lax.dot_general(k, rows, (((1,), (1,)), ((), ())), preferred_element_type=jnp.float32)
                p = jnp.exp2(st * c)
                if masked:
                    lane = lax.broadcasted_iota(jnp.int32, (1, w), 1)
                    at = lane // strip * period + offset + lane % strip
                    row = s + lax.broadcasted_iota(jnp.int32, (sub, 1), 0)
                    head = jnp.where(row <= at, p[:, :w], 0.0)
                    p = jnp.concatenate([head, p[:, w:]], axis=1) if bq - lo > w else head
                mass = jnp.sum(p.reshape(sub // 8, 8, bq - lo), axis=0)
                mixed = jnp.dot(values(blk, s, sub), p.astype(jnp.bfloat16), preferred_element_type=jnp.float32)
                if fresh:
                    l_ref[:, lo:] = mass
                    acc_ref[:, lo:] = mixed
                else:
                    l_ref[:, lo:] += mass
                    acc_ref[:, lo:] += mixed

        def body(j, _):
            for u in range(unroll):
                block(j * unroll + u, 0, False)
            return 0

        for t in range(nd):
            for later in groups.get(t, ()):
                landed(later)
            block(first + t, t * w, True, t == 0)
        lax.fori_loop(0, first // unroll, body, 0)
        total = jnp.sum(l_ref[...], axis=0, keepdims=True)
        o_ref[...] = (acc_ref[...] * (1.0 / total)).T.astype(jnp.bfloat16).reshape(o_ref.shape)
        fine = jnp.logical_and(jnp.min(total) > LOW, jnp.max(total) < HIGH)

        @pl.when(jnp.logical_not(fine))
        def _():
            qT_ref[...] = qv_ref[pl.ds(qi * devs, devs)].reshape(bq, D).astype(jnp.float32).T.astype(jnp.bfloat16)
            lane = lax.broadcasted_iota(jnp.int32, (1, bq), 1)
            at = qi * devs * period + lane // strip * period + offset + lane % strip

            def slow(blk, state):
                l, m = state
                st = jnp.dot(kv_ref[blk, :BK, :], qT_ref[...], preferred_element_type=jnp.float32) * c
                row = blk * BK + lax.broadcasted_iota(jnp.int32, (BK, 1), 0)
                st = jnp.where(row <= at, st, -jnp.inf)
                top = jnp.maximum(m, jnp.max(st, axis=0, keepdims=True))
                shrink = jnp.exp2(m - top)
                p = jnp.exp2(st - top)
                acc_ref[...] = acc_ref[...] * shrink + jnp.dot(
                    values(blk, 0, BK), p.astype(jnp.bfloat16), preferred_element_type=jnp.float32)
                return l * shrink + jnp.sum(p, axis=0, keepdims=True), top

            acc_ref[...] = jnp.zeros_like(acc_ref)
            start = (jnp.zeros((1, bq), jnp.float32), jnp.full((1, bq), -1e30, jnp.float32))
            l, _ = lax.fori_loop(0, first + nd, slow, start)
            o_ref[...] = (acc_ref[...] / l).T.astype(jnp.bfloat16).reshape(o_ref.shape)

    extra = () if out is None else (out,)
    anywhere = pl.BlockSpec(memory_space=pl.ANY)
    return pl.pallas_call(
        kernel, grid=(G // devs,),
        in_specs=[pl.BlockSpec(memory_space=pltpu.SMEM),
                  anywhere] + [anywhere] * (len(pieces) + len(extra)),
        out_specs=pl.BlockSpec((devs, strip, D), lambda i: (i, which, 0)),
        out_shape=jax.ShapeDtypeStruct((G, period, D), jnp.bfloat16),
        input_output_aliases={2 + len(pieces): 0} if extra else {},
        scratch_shapes=[pltpu.VMEM((D, bq), jnp.bfloat16), pltpu.VMEM((D, bq), jnp.float32),
                        pltpu.VMEM((8, bq), jnp.float32), pltpu.VMEM((blocks, 2 * BK, D), jnp.bfloat16),
                        pltpu.VMEM((G, strip, D), jnp.bfloat16),
                        pltpu.SemaphoreType.DMA((blocks + 1,))],
        compiler_params=pltpu.CompilerParams(vmem_limit_bytes=24 * 2**20),
        name="attn",
    )(where, *(pltpu.with_memory_space_constraint(piece, pltpu.HBM) for piece in (q, *pieces)), *extra)


def shards(queries, keys, values):
    rows, heads_all, width = queries.shape
    key_heads = keys.shape[1]
    group = heads_all // key_heads
    x, _, core, _ = (lax.axis_index(a) for a in AXES)
    start_row = lax.axis_index(AXES) * rows
    positions = start_row + jnp.arange(rows, dtype=jnp.int32)

    angles = positions.astype(jnp.float32)[:, None] * jnp.tile(frequencies(width), 2)[None, :]
    cosine = jnp.cos(angles)
    signed_sine = jnp.sin(angles) * jnp.where(jnp.arange(width) < width // 2, -1.0, 1.0)

    pair = prepare_pair(keys, values, cosine, signed_sine)
    pair = lax.all_to_all(pair, ("yl", "sy"), split_axis=0, concat_axis=0, tiled=True)
    pair = pair.swapaxes(0, 1).reshape(2, 2, -1, width)
    block = pair.shape[2]
    own_values = pair[1].reshape(2, block // 128, 128, width).swapaxes(2, 3).reshape(2, block, width)
    c = jnp.concatenate([pair[0], own_values], axis=1)
    ahead = [(i, (i + 1) % 4) for i in range(4)]
    behind = [(i, (i - 1) % 4) for i in range(4)]
    swap = [(0, 1), (1, 0)]
    u = lax.ppermute(c, "x", ahead)
    v = lax.ppermute(c, "x", behind)
    h = lax.ppermute(u[0:1], "x", ahead)
    g = lax.ppermute(v[1:2], "x", behind)
    pieces = []
    for piece in (c, u, v, h, g):
        pieces += [piece, lax.ppermute(piece, "core", swap)]
    where = jnp.stack([x, core]).astype(jnp.int32)

    ordered = prepare_queries(queries, cosine, signed_sine, group)
    arrived = []
    for n in range(CHUNKS):
        arrived.append(lax.all_to_all(ordered[n], AXES, split_axis=0, concat_axis=0, tiled=True))
    out = None
    for n in range(CHUNKS):
        out = attn(arrived[n], pieces, where, out, bq=TILE, period=rows, which=n)
    merged = lax.all_to_all(out.swapaxes(0, 1), AXES, split_axis=1, concat_axis=1, tiled=True)
    return (
        merged.reshape(rows, group, key_heads, width)
        .transpose(0, 2, 1, 3)
        .reshape(rows, heads_all, width)
    )


def solution(mesh):
    finer = Mesh(mesh.devices.reshape(4, 2, 2, 8), AXES)
    placed = P(AXES, None, None)

    return jax.shard_map(shards, mesh=finer, in_specs=(placed,) * 3, out_specs=placed, check_vma=False)
```

```python
import math

import jax
import jax.numpy as jnp
from jax import lax
from jax.experimental import pallas as pl
from jax.experimental.pallas import tpu as pltpu
from jax.sharding import Mesh, PartitionSpec as P


LOG2E = 1.4426950408889634
LOW, HIGH = 2.0**-80, 2.0**100
CHUNKS = 2
TILE = 2048
GROUPS = {8: {0: (0,), 1: tuple(range(1, 8))}}
AXES = ("x", "yl", "core", "sy")


def frequencies(head_width):
    half_index = jnp.arange(head_width // 2, dtype=jnp.float32)
    base_rate = jnp.power(jnp.float32(500000.0), -2.0 * half_index / head_width)
    wavelen = 2.0 * math.pi / base_rate
    smooth = (8192.0 / wavelen - 1.0) / 3.0
    blended = (1.0 - smooth) * base_rate / 8.0 + smooth * base_rate
    return jnp.where(
        wavelen < 2048.0, base_rate, jnp.where(wavelen > 8192.0, base_rate / 8.0, blended)
    )


def turned(head, cosine, signed_sine):
    return head * cosine + pltpu.roll(head, head.shape[-1] // 2, 1) * signed_sine


def prepare_pair(keys, values, cosine, signed_sine):
    rows, heads, width = keys.shape

    def kernel(k_ref, v_ref, cos_ref, sin_ref, o_ref, kf_ref, vf_ref):
        kf_ref[...] = k_ref[...].astype(jnp.float32)
        vf_ref[...] = v_ref[...].astype(jnp.float32)
        for h in range(heads):
            key = turned(kf_ref[:, h, :], cos_ref[...], sin_ref[...]).astype(jnp.bfloat16)
            value = vf_ref[:, h, :].astype(jnp.bfloat16)
            for half in (0, heads):
                o_ref[half + h, 0] = key
                o_ref[half + h, 1] = value

    wide = pltpu.VMEM((rows, heads, width), jnp.float32)
    return pl.pallas_call(
        kernel, out_shape=jax.ShapeDtypeStruct((2 * heads, 2, rows, width), jnp.bfloat16),
        scratch_shapes=[wide, wide], name="pair",
    )(keys, values, cosine, signed_sine)


def prepare_queries(queries, cosine, signed_sine, group):
    rows, heads, width = queries.shape
    strip = rows // CHUNKS

    def kernel(q_ref, cos_ref, sin_ref, *rest):
        outs, wide_ref = rest[:-1], rest[-1]
        wide_ref[...] = q_ref[...].astype(jnp.float32)
        for h in range(group):
            head = turned(wide_ref[:, h, :], cos_ref[...], sin_ref[...]).astype(jnp.bfloat16)
            for n, o_ref in enumerate(outs):
                o_ref[h, 0] = head[n * strip:(n + 1) * strip]

    table = pl.BlockSpec((rows, width), lambda g: (0, 0))
    parts = pl.pallas_call(
        kernel, grid=(heads // group,),
        in_specs=[pl.BlockSpec((rows, group, width), lambda g: (0, g, 0)), table, table],
        out_specs=[pl.BlockSpec((group, 1, strip, width), lambda g: (0, g, 0, 0))] * CHUNKS,
        out_shape=[jax.ShapeDtypeStruct((group, heads // group, strip, width), jnp.bfloat16)] * CHUNKS,
        scratch_shapes=[pltpu.VMEM((rows, group, width), jnp.float32)], name="queries",
    )(queries, cosine, signed_sine)
    return [part.reshape(heads, strip, width) for part in parts]


def attn(q, pieces, where, out, *, bq, period, which, sub=512, unroll=4):
    G, strip, D = q.shape
    BK = pieces[0].shape[1] // 2
    blocks = G * period // BK
    c = LOG2E / math.sqrt(D)
    devs = bq // strip
    nd = devs * period // BK
    w = bq // nd
    offset = which * strip
    groups = GROUPS[nd]

    def kernel(where_ref, q_ref, c_ref, cc_ref, u_ref, cu_ref, v_ref, cv_ref, h_ref, ch_ref, g_ref, cg_ref,
               *rest):
        o_ref, qT_ref, acc_ref, l_ref, kv_ref, qv_ref, sems = rest[-7:]
        qi = pl.program_id(0)
        first = qi * nd

        @pl.when(qi == 0)
        def _():
            pltpu.make_async_copy(q_ref, qv_ref, sems.at[blocks]).start()
            x, core = where_ref[0], where_ref[1]
            for plane in range(4):
                for step, refs in ((0, (c_ref, cc_ref)), (3, (u_ref, cu_ref)), (1, (v_ref, cv_ref)),
                                   (2, ((h_ref, g_ref), (ch_ref, cg_ref)))):
                    @pl.when(lax.rem(x + step, 4) == plane)
                    def _():
                        for yl in (0, 1):
                            for other in (0, 1):
                                src = refs[other][yl].at[0] if step == 2 else refs[other].at[yl]
                                b = plane * 4 + yl * 2 + lax.rem(core + other, 2)
                                pltpu.make_async_copy(src, kv_ref.at[b], sems.at[b]).start()

        @pl.when(qi == 0)
        def _():
            pltpu.make_async_copy(q_ref, qv_ref, sems.at[blocks]).wait()

        def landed(t):
            pltpu.make_async_copy(c_ref.at[0], kv_ref.at[first + t], sems.at[first + t]).wait()


        def values(blk, lo, n):
            return jnp.concatenate(
                [kv_ref[blk, BK + lo + t * 128: BK + lo + (t + 1) * 128, :] for t in range(n // 128)], axis=1)

        def block(blk, lo, masked, fresh=False):
            for s in range(0, BK, sub):
                k = kv_ref[blk, s:s + sub, :]
                rows = qv_ref[pl.ds(qi * devs + lo // strip, devs - lo // strip)].reshape(bq - lo, D)
                st = lax.dot_general(k, rows, (((1,), (1,)), ((), ())), preferred_element_type=jnp.float32)
                p = jnp.exp2(st * c)
                if masked:
                    lane = lax.broadcasted_iota(jnp.int32, (1, w), 1)
                    at = lane // strip * period + offset + lane % strip
                    row = s + lax.broadcasted_iota(jnp.int32, (sub, 1), 0)
                    head = jnp.where(row <= at, p[:, :w], 0.0)
                    p = jnp.concatenate([head, p[:, w:]], axis=1) if bq - lo > w else head
                mass = jnp.sum(p.reshape(sub // 8, 8, bq - lo), axis=0)
                mixed = jnp.dot(values(blk, s, sub), p.astype(jnp.bfloat16), preferred_element_type=jnp.float32)
                if fresh:
                    l_ref[:, lo:] = mass
                    acc_ref[:, lo:] = mixed
                else:
                    l_ref[:, lo:] += mass
                    acc_ref[:, lo:] += mixed

        def body(j, _):
            for u in range(unroll):
                block(j * unroll + u, 0, False)
            return 0

        for t in range(nd):
            for later in groups.get(t, ()):
                landed(later)
            block(first + t, t * w, True, t == 0)
        lax.fori_loop(0, first // unroll, body, 0)
        total = jnp.sum(l_ref[...], axis=0, keepdims=True)
        o_ref[...] = (acc_ref[...] * (1.0 / total)).T.astype(jnp.bfloat16).reshape(o_ref.shape)
        fine = jnp.logical_and(jnp.min(total) > LOW, jnp.max(total) < HIGH)

        @pl.when(jnp.logical_not(fine))
        def _():
            qT_ref[...] = qv_ref[pl.ds(qi * devs, devs)].reshape(bq, D).astype(jnp.float32).T.astype(jnp.bfloat16)
            lane = lax.broadcasted_iota(jnp.int32, (1, bq), 1)
            at = qi * devs * period + lane // strip * period + offset + lane % strip

            def slow(blk, state):
                l, m = state
                st = jnp.dot(kv_ref[blk, :BK, :], qT_ref[...], preferred_element_type=jnp.float32) * c
                row = blk * BK + lax.broadcasted_iota(jnp.int32, (BK, 1), 0)
                st = jnp.where(row <= at, st, -jnp.inf)
                top = jnp.maximum(m, jnp.max(st, axis=0, keepdims=True))
                shrink = jnp.exp2(m - top)
                p = jnp.exp2(st - top)
                acc_ref[...] = acc_ref[...] * shrink + jnp.dot(
                    values(blk, 0, BK), p.astype(jnp.bfloat16), preferred_element_type=jnp.float32)
                return l * shrink + jnp.sum(p, axis=0, keepdims=True), top

            acc_ref[...] = jnp.zeros_like(acc_ref)
            start = (jnp.zeros((1, bq), jnp.float32), jnp.full((1, bq), -1e30, jnp.float32))
            l, _ = lax.fori_loop(0, first + nd, slow, start)
            o_ref[...] = (acc_ref[...] / l).T.astype(jnp.bfloat16).reshape(o_ref.shape)

    extra = () if out is None else (out,)
    anywhere = pl.BlockSpec(memory_space=pl.ANY)
    return pl.pallas_call(
        kernel, grid=(G // devs,),
        in_specs=[pl.BlockSpec(memory_space=pltpu.SMEM),
                  anywhere] + [anywhere] * (len(pieces) + len(extra)),
        out_specs=pl.BlockSpec((devs, strip, D), lambda i: (i, which, 0)),
        out_shape=jax.ShapeDtypeStruct((G, period, D), jnp.bfloat16),
        input_output_aliases={2 + len(pieces): 0} if extra else {},
        scratch_shapes=[pltpu.VMEM((D, bq), jnp.bfloat16), pltpu.VMEM((D, bq), jnp.float32),
                        pltpu.VMEM((8, bq), jnp.float32), pltpu.VMEM((blocks, 2 * BK, D), jnp.bfloat16),
                        pltpu.VMEM((G, strip, D), jnp.bfloat16),
                        pltpu.SemaphoreType.DMA((blocks + 1,))],
        compiler_params=pltpu.CompilerParams(vmem_limit_bytes=24 * 2**20),
        name="attn",
    )(where, *(pltpu.with_memory_space_constraint(piece, pltpu.HBM) for piece in (q, *pieces)), *extra)


def shards(queries, keys, values):
    rows, heads_all, width = queries.shape
    key_heads = keys.shape[1]
    group = heads_all // key_heads
    x, _, core, _ = (lax.axis_index(a) for a in AXES)
    start_row = lax.axis_index(AXES) * rows
    positions = start_row + jnp.arange(rows, dtype=jnp.int32)

    angles = positions.astype(jnp.float32)[:, None] * jnp.tile(frequencies(width), 2)[None, :]
    cosine = jnp.cos(angles)
    signed_sine = jnp.sin(angles) * jnp.where(jnp.arange(width) < width // 2, -1.0, 1.0)

    pair = prepare_pair(keys, values, cosine, signed_sine)
    pair = lax.all_to_all(pair, ("yl", "sy"), split_axis=0, concat_axis=0, tiled=True)
    pair = pair.swapaxes(0, 1).reshape(2, 2, -1, width)
    block = pair.shape[2]
    own_values = pair[1].reshape(2, block // 128, 128, width).swapaxes(2, 3).reshape(2, block, width)
    c = jnp.concatenate([pair[0], own_values], axis=1)
    ahead = [(i, (i + 1) % 4) for i in range(4)]
    behind = [(i, (i - 1) % 4) for i in range(4)]
    swap = [(0, 1), (1, 0)]
    u = lax.ppermute(c, "x", ahead)
    v = lax.ppermute(c, "x", behind)
    near = []
    for piece in (c, u, v):
        near += [piece, lax.ppermute(piece, "core", swap)]
    far = []
    for source, half, way in ((near[2], 0, ahead), (near[4], 1, behind), (near[3], 0, ahead), (near[5], 1, behind)):
        far.append(lax.ppermute(source[half:half + 1], "x", way))
    pieces = near + [far[0], far[2], far[1], far[3]]
    where = jnp.stack([x, core]).astype(jnp.int32)

    ordered = prepare_queries(queries, cosine, signed_sine, group)
    arrived = []
    for n in range(CHUNKS):
        arrived.append(lax.all_to_all(ordered[n], AXES, split_axis=0, concat_axis=0, tiled=True))
    out = None
    for n in range(CHUNKS):
        out = attn(arrived[n], pieces, where, out, bq=TILE, period=rows, which=n)
    merged = lax.all_to_all(out.swapaxes(0, 1), AXES, split_axis=1, concat_axis=1, tiled=True)
    return (
        merged.reshape(rows, group, key_heads, width)
        .transpose(0, 2, 1, 3)
        .reshape(rows, heads_all, width)
    )


def solution(mesh):
    finer = Mesh(mesh.devices.reshape(4, 2, 2, 8), AXES)
    placed = P(AXES, None, None)

    return jax.shard_map(shards, mesh=finer, in_specs=(placed,) * 3, out_specs=placed, check_vma=False)
```

```python
import math

import jax
import jax.numpy as jnp
from jax import lax
from jax.experimental import pallas as pl
from jax.experimental.pallas import tpu as pltpu
from jax.sharding import Mesh, PartitionSpec as P


LOG2E = 1.4426950408889634
LOW, HIGH = 2.0**-80, 2.0**100
CHUNKS = 2
TILE = 2048
GROUPS = {8: {0: (0,), 1: tuple(range(1, 8))}}
AXES = ("x", "yl", "core", "sy")


def frequencies(head_width):
    half_index = jnp.arange(head_width // 2, dtype=jnp.float32)
    base_rate = jnp.power(jnp.float32(500000.0), -2.0 * half_index / head_width)
    wavelen = 2.0 * math.pi / base_rate
    smooth = (8192.0 / wavelen - 1.0) / 3.0
    blended = (1.0 - smooth) * base_rate / 8.0 + smooth * base_rate
    return jnp.where(
        wavelen < 2048.0, base_rate, jnp.where(wavelen > 8192.0, base_rate / 8.0, blended)
    )


def turned(head, cosine, signed_sine):
    return head * cosine + pltpu.roll(head, head.shape[-1] // 2, 1) * signed_sine


def prepare_pair(keys, values, cosine, signed_sine):
    rows, heads, width = keys.shape

    def kernel(k_ref, v_ref, cos_ref, sin_ref, o_ref, kf_ref, vf_ref):
        kf_ref[...] = k_ref[...].astype(jnp.float32)
        vf_ref[...] = v_ref[...].astype(jnp.float32)
        for h in range(heads):
            key = turned(kf_ref[:, h, :], cos_ref[...], sin_ref[...]).astype(jnp.bfloat16)
            value = vf_ref[:, h, :].astype(jnp.bfloat16)
            for half in (0, heads):
                o_ref[half + h, 0] = key
                o_ref[half + h, 1] = value

    wide = pltpu.VMEM((rows, heads, width), jnp.float32)
    return pl.pallas_call(
        kernel, out_shape=jax.ShapeDtypeStruct((2 * heads, 2, rows, width), jnp.bfloat16),
        scratch_shapes=[wide, wide], name="pair",
    )(keys, values, cosine, signed_sine)


def prepare_queries(queries, cosine, signed_sine, group):
    rows, heads, width = queries.shape
    strip = rows // CHUNKS

    def kernel(q_ref, cos_ref, sin_ref, *rest):
        outs, wide_ref = rest[:-1], rest[-1]
        wide_ref[...] = q_ref[...].astype(jnp.float32)
        for h in range(group):
            head = turned(wide_ref[:, h, :], cos_ref[...], sin_ref[...]).astype(jnp.bfloat16)
            for n, o_ref in enumerate(outs):
                o_ref[h, 0] = head[n * strip:(n + 1) * strip]

    table = pl.BlockSpec((rows, width), lambda g: (0, 0))
    parts = pl.pallas_call(
        kernel, grid=(heads // group,),
        in_specs=[pl.BlockSpec((rows, group, width), lambda g: (0, g, 0)), table, table],
        out_specs=[pl.BlockSpec((group, 1, strip, width), lambda g: (0, g, 0, 0))] * CHUNKS,
        out_shape=[jax.ShapeDtypeStruct((group, heads // group, strip, width), jnp.bfloat16)] * CHUNKS,
        scratch_shapes=[pltpu.VMEM((rows, group, width), jnp.float32)], name="queries",
    )(queries, cosine, signed_sine)
    return [part.reshape(heads, strip, width) for part in parts]


def attn(q, pieces, where, *, bq, period, which, sub=512, unroll=4):
    G, strip, D = q.shape
    BK = pieces[0].shape[1] // 2
    blocks = G * period // BK
    c = LOG2E / math.sqrt(D)
    devs = bq // strip
    nd = devs * period // BK
    w = bq // nd
    offset = which * strip
    groups = GROUPS[nd]

    def kernel(where_ref, q_ref, c_ref, cc_ref, u_ref, cu_ref, v_ref, cv_ref, h_ref, ch_ref, g_ref, cg_ref,
               *rest):
        o_ref, qT_ref, acc_ref, l_ref, kv_ref, qv_ref, sems = rest[-7:]
        qi = pl.program_id(0)
        first = qi * nd

        @pl.when(qi == 0)
        def _():
            pltpu.make_async_copy(q_ref, qv_ref, sems.at[blocks]).start()
            x, core = where_ref[0], where_ref[1]
            for plane in range(4):
                for step, refs in ((0, (c_ref, cc_ref)), (3, (u_ref, cu_ref)), (1, (v_ref, cv_ref)),
                                   (2, ((h_ref, g_ref), (ch_ref, cg_ref)))):
                    @pl.when(lax.rem(x + step, 4) == plane)
                    def _():
                        for yl in (0, 1):
                            for other in (0, 1):
                                src = refs[other][yl].at[0] if step == 2 else refs[other].at[yl]
                                b = plane * 4 + yl * 2 + lax.rem(core + other, 2)
                                pltpu.make_async_copy(src, kv_ref.at[b], sems.at[b]).start()

        @pl.when(qi == 0)
        def _():
            pltpu.make_async_copy(q_ref, qv_ref, sems.at[blocks]).wait()

        def landed(t):
            pltpu.make_async_copy(c_ref.at[0], kv_ref.at[first + t], sems.at[first + t]).wait()


        def values(blk, lo, n):
            return jnp.concatenate(
                [kv_ref[blk, BK + lo + t * 128: BK + lo + (t + 1) * 128, :] for t in range(n // 128)], axis=1)

        def block(blk, lo, masked, fresh=False):
            for s in range(0, BK, sub):
                k = kv_ref[blk, s:s + sub, :]
                rows = qv_ref[pl.ds(qi * devs + lo // strip, devs - lo // strip)].reshape(bq - lo, D)
                st = lax.dot_general(k, rows, (((1,), (1,)), ((), ())), preferred_element_type=jnp.float32)
                p = jnp.exp2(st * c)
                if masked:
                    lane = lax.broadcasted_iota(jnp.int32, (1, w), 1)
                    at = lane // strip * period + offset + lane % strip
                    row = s + lax.broadcasted_iota(jnp.int32, (sub, 1), 0)
                    head = jnp.where(row <= at, p[:, :w], 0.0)
                    p = jnp.concatenate([head, p[:, w:]], axis=1) if bq - lo > w else head
                mass = jnp.sum(p.reshape(sub // 8, 8, bq - lo), axis=0)
                mixed = jnp.dot(values(blk, s, sub), p.astype(jnp.bfloat16), preferred_element_type=jnp.float32)
                if fresh:
                    l_ref[:, lo:] = mass
                    acc_ref[:, lo:] = mixed
                else:
                    l_ref[:, lo:] += mass
                    acc_ref[:, lo:] += mixed

        def body(j, _):
            for u in range(unroll):
                block(j * unroll + u, 0, False)
            return 0

        for t in range(nd):
            for later in groups.get(t, ()):
                landed(later)
            block(first + t, t * w, True, t == 0)
        lax.fori_loop(0, first // unroll, body, 0)
        total = jnp.sum(l_ref[...], axis=0, keepdims=True)
        o_ref[...] = (acc_ref[...] * (1.0 / total)).T.astype(jnp.bfloat16).reshape(o_ref.shape)
        fine = jnp.logical_and(jnp.min(total) > LOW, jnp.max(total) < HIGH)

        @pl.when(jnp.logical_not(fine))
        def _():
            qT_ref[...] = qv_ref[pl.ds(qi * devs, devs)].reshape(bq, D).astype(jnp.float32).T.astype(jnp.bfloat16)
            lane = lax.broadcasted_iota(jnp.int32, (1, bq), 1)
            at = qi * devs * period + lane // strip * period + offset + lane % strip

            def slow(blk, state):
                l, m = state
                st = jnp.dot(kv_ref[blk, :BK, :], qT_ref[...], preferred_element_type=jnp.float32) * c
                row = blk * BK + lax.broadcasted_iota(jnp.int32, (BK, 1), 0)
                st = jnp.where(row <= at, st, -jnp.inf)
                top = jnp.maximum(m, jnp.max(st, axis=0, keepdims=True))
                shrink = jnp.exp2(m - top)
                p = jnp.exp2(st - top)
                acc_ref[...] = acc_ref[...] * shrink + jnp.dot(
                    values(blk, 0, BK), p.astype(jnp.bfloat16), preferred_element_type=jnp.float32)
                return l * shrink + jnp.sum(p, axis=0, keepdims=True), top

            acc_ref[...] = jnp.zeros_like(acc_ref)
            start = (jnp.zeros((1, bq), jnp.float32), jnp.full((1, bq), -1e30, jnp.float32))
            l, _ = lax.fori_loop(0, first + nd, slow, start)
            o_ref[...] = (acc_ref[...] / l).T.astype(jnp.bfloat16).reshape(o_ref.shape)

    anywhere = pl.BlockSpec(memory_space=pl.ANY)
    return pl.pallas_call(
        kernel, grid=(G // devs,),
        in_specs=[pl.BlockSpec(memory_space=pltpu.SMEM),
                  anywhere] + [anywhere] * len(pieces),
        out_specs=pl.BlockSpec((devs, strip, D), lambda i: (i, 0, 0)),
        out_shape=jax.ShapeDtypeStruct((G, strip, D), jnp.bfloat16),
        scratch_shapes=[pltpu.VMEM((D, bq), jnp.bfloat16), pltpu.VMEM((D, bq), jnp.float32),
                        pltpu.VMEM((8, bq), jnp.float32), pltpu.VMEM((blocks, 2 * BK, D), jnp.bfloat16),
                        pltpu.VMEM((G, strip, D), jnp.bfloat16),
                        pltpu.SemaphoreType.DMA((blocks + 1,))],
        compiler_params=pltpu.CompilerParams(vmem_limit_bytes=24 * 2**20),
        name="attn",
    )(where, *(pltpu.with_memory_space_constraint(piece, pltpu.HBM) for piece in (q, *pieces)))


def shards(queries, keys, values):
    rows, heads_all, width = queries.shape
    key_heads = keys.shape[1]
    group = heads_all // key_heads
    x, _, core, _ = (lax.axis_index(a) for a in AXES)
    start_row = lax.axis_index(AXES) * rows
    positions = start_row + jnp.arange(rows, dtype=jnp.int32)

    angles = positions.astype(jnp.float32)[:, None] * jnp.tile(frequencies(width), 2)[None, :]
    cosine = jnp.cos(angles)
    signed_sine = jnp.sin(angles) * jnp.where(jnp.arange(width) < width // 2, -1.0, 1.0)

    pair = prepare_pair(keys, values, cosine, signed_sine)
    pair = lax.all_to_all(pair, ("yl", "sy"), split_axis=0, concat_axis=0, tiled=True)
    pair = pair.swapaxes(0, 1).reshape(2, 2, -1, width)
    block = pair.shape[2]
    own_values = pair[1].reshape(2, block // 128, 128, width).swapaxes(2, 3).reshape(2, block, width)
    c = jnp.concatenate([pair[0], own_values], axis=1)
    ahead = [(i, (i + 1) % 4) for i in range(4)]
    behind = [(i, (i - 1) % 4) for i in range(4)]
    swap = [(0, 1), (1, 0)]
    u = lax.ppermute(c, "x", ahead)
    v = lax.ppermute(c, "x", behind)
    near = []
    for piece in (c, u, v):
        near += [piece, lax.ppermute(piece, "core", swap)]
    far = []
    for source, half, way in ((near[2], 0, ahead), (near[4], 1, behind), (near[3], 0, ahead), (near[5], 1, behind)):
        far.append(lax.ppermute(source[half:half + 1], "x", way))
    pieces = near + [far[0], far[2], far[1], far[3]]
    where = jnp.stack([x, core]).astype(jnp.int32)

    ordered = prepare_queries(queries, cosine, signed_sine, group)
    arrived = []
    for n in range(CHUNKS):
        arrived.append(lax.all_to_all(ordered[n], AXES, split_axis=0, concat_axis=0, tiled=True))
    halves = []
    for n in range(CHUNKS):
        done = attn(arrived[n], pieces, where, bq=TILE, period=rows, which=n)
        back = lax.all_to_all(done, AXES, split_axis=0, concat_axis=0, tiled=True)
        back = back.reshape(group, key_heads, -1, width).transpose(2, 1, 0, 3)
        halves.append(back.reshape(-1, heads_all, width))
    return jnp.concatenate(halves, axis=0)


def solution(mesh):
    finer = Mesh(mesh.devices.reshape(4, 2, 2, 8), AXES)
    placed = P(AXES, None, None)

    return jax.shard_map(shards, mesh=finer, in_specs=(placed,) * 3, out_specs=placed, check_vma=False)
```

```python
import math

import jax
import jax.numpy as jnp
from jax import lax
from jax.experimental import pallas as pl
from jax.experimental.pallas import tpu as pltpu
from jax.sharding import Mesh, PartitionSpec as P


LOG2E = 1.4426950408889634
LOW, HIGH = 2.0**-80, 2.0**100
CHUNKS = 2
TILE = 2048
GROUPS = {8: {0: (0,), 1: tuple(range(1, 8))}}
AXES = ("x", "yl", "core", "sy")


def frequencies(head_width):
    half_index = jnp.arange(head_width // 2, dtype=jnp.float32)
    base_rate = jnp.power(jnp.float32(500000.0), -2.0 * half_index / head_width)
    wavelen = 2.0 * math.pi / base_rate
    smooth = (8192.0 / wavelen - 1.0) / 3.0
    blended = (1.0 - smooth) * base_rate / 8.0 + smooth * base_rate
    return jnp.where(
        wavelen < 2048.0, base_rate, jnp.where(wavelen > 8192.0, base_rate / 8.0, blended)
    )


def turned(head, cosine, signed_sine):
    return head * cosine + pltpu.roll(head, head.shape[-1] // 2, 1) * signed_sine


def prepare_pair(keys, values, cosine, signed_sine):
    rows, heads, width = keys.shape

    def kernel(k_ref, v_ref, cos_ref, sin_ref, o_ref, kf_ref, vf_ref):
        kf_ref[...] = k_ref[...].astype(jnp.float32)
        vf_ref[...] = v_ref[...].astype(jnp.float32)
        for h in range(heads):
            key = turned(kf_ref[:, h, :], cos_ref[...], sin_ref[...]).astype(jnp.bfloat16)
            value = vf_ref[:, h, :].astype(jnp.bfloat16)
            for half in (0, heads):
                o_ref[half + h, 0] = key
                o_ref[half + h, 1] = value

    wide = pltpu.VMEM((rows, heads, width), jnp.float32)
    return pl.pallas_call(
        kernel, out_shape=jax.ShapeDtypeStruct((2 * heads, 2, rows, width), jnp.bfloat16),
        scratch_shapes=[wide, wide], name="pair",
    )(keys, values, cosine, signed_sine)


def prepare_queries(queries, cosine, signed_sine, group):
    rows, heads, width = queries.shape
    strip = rows // CHUNKS

    def kernel(q_ref, cos_ref, sin_ref, *rest):
        outs, wide_ref = rest[:-1], rest[-1]
        wide_ref[...] = q_ref[...].astype(jnp.float32)
        for h in range(group):
            head = turned(wide_ref[:, h, :], cos_ref[...], sin_ref[...]).astype(jnp.bfloat16)
            for n, o_ref in enumerate(outs):
                o_ref[h, 0] = head[n * strip:(n + 1) * strip]

    table = pl.BlockSpec((rows, width), lambda g: (0, 0))
    parts = pl.pallas_call(
        kernel, grid=(heads // group,),
        in_specs=[pl.BlockSpec((rows, group, width), lambda g: (0, g, 0)), table, table],
        out_specs=[pl.BlockSpec((group, 1, strip, width), lambda g: (0, g, 0, 0))] * CHUNKS,
        out_shape=[jax.ShapeDtypeStruct((group, heads // group, strip, width), jnp.bfloat16)] * CHUNKS,
        scratch_shapes=[pltpu.VMEM((rows, group, width), jnp.float32)], name="queries",
    )(queries, cosine, signed_sine)
    return [part.reshape(heads, strip, width) for part in parts]


def attn(q, pieces, where, *, bq, period, which, sub=512, unroll=4):
    G, strip, D = q.shape
    BK = pieces[0].shape[1] // 2
    blocks = G * period // BK
    c = LOG2E / math.sqrt(D)
    devs = bq // strip
    nd = devs * period // BK
    w = bq // nd
    offset = which * strip
    groups = GROUPS[nd]

    def kernel(where_ref, q_ref, c_ref, cc_ref, u_ref, cu_ref, v_ref, cv_ref, h_ref, ch_ref, g_ref, cg_ref,
               *rest):
        o_ref, qT_ref, acc_ref, l_ref, kv_ref, qv_ref, sems = rest[-7:]
        qi = pl.program_id(0)
        first = qi * nd

        @pl.when(qi == 0)
        def _():
            pltpu.make_async_copy(q_ref, qv_ref, sems.at[blocks]).start()
            x, core = where_ref[0], where_ref[1]
            for plane in range(4):
                for step, refs in ((0, (c_ref, cc_ref)), (3, (u_ref, cu_ref)), (1, (v_ref, cv_ref)),
                                   (2, ((h_ref, g_ref), (ch_ref, cg_ref)))):
                    @pl.when(lax.rem(x + step, 4) == plane)
                    def _():
                        for yl in (0, 1):
                            for other in (0, 1):
                                src = refs[other][yl].at[0] if step == 2 else refs[other].at[yl]
                                b = plane * 4 + yl * 2 + lax.rem(core + other, 2)
                                pltpu.make_async_copy(src, kv_ref.at[b], sems.at[b]).start()

        @pl.when(qi == 0)
        def _():
            pltpu.make_async_copy(q_ref, qv_ref, sems.at[blocks]).wait()

        def landed(t):
            pltpu.make_async_copy(c_ref.at[0], kv_ref.at[first + t], sems.at[first + t]).wait()


        def values(blk, lo, n):
            return jnp.concatenate(
                [kv_ref[blk, BK + lo + t * 128: BK + lo + (t + 1) * 128, :] for t in range(n // 128)], axis=1)

        def block(blk, lo, masked, fresh=False):
            for s in range(0, BK, sub):
                k = kv_ref[blk, s:s + sub, :]
                rows = qv_ref[pl.ds(qi * devs + lo // strip, devs - lo // strip)].reshape(bq - lo, D)
                st = lax.dot_general(k, rows, (((1,), (1,)), ((), ())), preferred_element_type=jnp.float32)
                p = jnp.exp2(st * c)
                if masked:
                    lane = lax.broadcasted_iota(jnp.int32, (1, w), 1)
                    at = lane // strip * period + offset + lane % strip
                    row = s + lax.broadcasted_iota(jnp.int32, (sub, 1), 0)
                    head = jnp.where(row <= at, p[:, :w], 0.0)
                    p = jnp.concatenate([head, p[:, w:]], axis=1) if bq - lo > w else head
                mass = jnp.sum(p.reshape(sub // 8, 8, bq - lo), axis=0)
                mixed = jnp.dot(values(blk, s, sub), p.astype(jnp.bfloat16), preferred_element_type=jnp.float32)
                if fresh:
                    l_ref[:, lo:] = mass
                    acc_ref[:, lo:] = mixed
                else:
                    l_ref[:, lo:] += mass
                    acc_ref[:, lo:] += mixed

        def body(j, _):
            for u in range(unroll):
                block(j * unroll + u, 0, False)
            return 0

        for t in range(nd):
            for later in groups.get(t, ()):
                landed(later)
            block(first + t, t * w, True, t == 0)
        lax.fori_loop(0, first // unroll, body, 0)
        total = jnp.sum(l_ref[...], axis=0, keepdims=True)
        o_ref[...] = (acc_ref[...] * (1.0 / total)).T.astype(jnp.bfloat16).reshape(o_ref.shape)
        fine = jnp.logical_and(jnp.min(total) > LOW, jnp.max(total) < HIGH)

        @pl.when(jnp.logical_not(fine))
        def _():
            qT_ref[...] = qv_ref[pl.ds(qi * devs, devs)].reshape(bq, D).astype(jnp.float32).T.astype(jnp.bfloat16)
            lane = lax.broadcasted_iota(jnp.int32, (1, bq), 1)
            at = qi * devs * period + lane // strip * period + offset + lane % strip

            def slow(blk, state):
                l, m = state
                st = jnp.dot(kv_ref[blk, :BK, :], qT_ref[...], preferred_element_type=jnp.float32) * c
                row = blk * BK + lax.broadcasted_iota(jnp.int32, (BK, 1), 0)
                st = jnp.where(row <= at, st, -jnp.inf)
                top = jnp.maximum(m, jnp.max(st, axis=0, keepdims=True))
                shrink = jnp.exp2(m - top)
                p = jnp.exp2(st - top)
                acc_ref[...] = acc_ref[...] * shrink + jnp.dot(
                    values(blk, 0, BK), p.astype(jnp.bfloat16), preferred_element_type=jnp.float32)
                return l * shrink + jnp.sum(p, axis=0, keepdims=True), top

            acc_ref[...] = jnp.zeros_like(acc_ref)
            start = (jnp.zeros((1, bq), jnp.float32), jnp.full((1, bq), -1e30, jnp.float32))
            l, _ = lax.fori_loop(0, first + nd, slow, start)
            o_ref[...] = (acc_ref[...] / l).T.astype(jnp.bfloat16).reshape(o_ref.shape)

    anywhere = pl.BlockSpec(memory_space=pl.ANY)
    return pl.pallas_call(
        kernel, grid=(G // devs,),
        in_specs=[pl.BlockSpec(memory_space=pltpu.SMEM),
                  anywhere] + [anywhere] * len(pieces),
        out_specs=pl.BlockSpec((devs, strip, D), lambda i: (i, 0, 0)),
        out_shape=jax.ShapeDtypeStruct((G, strip, D), jnp.bfloat16),
        scratch_shapes=[pltpu.VMEM((D, bq), jnp.bfloat16), pltpu.VMEM((D, bq), jnp.float32),
                        pltpu.VMEM((8, bq), jnp.float32), pltpu.VMEM((blocks, 2 * BK, D), jnp.bfloat16),
                        pltpu.VMEM((G, strip, D), jnp.bfloat16),
                        pltpu.SemaphoreType.DMA((blocks + 1,))],
        compiler_params=pltpu.CompilerParams(vmem_limit_bytes=24 * 2**20),
        name="attn",
    )(where, *(pltpu.with_memory_space_constraint(piece, pltpu.HBM) for piece in (q, *pieces)))


def shards(queries, keys, values):
    rows, heads_all, width = queries.shape
    key_heads = keys.shape[1]
    group = heads_all // key_heads
    x, _, core, _ = (lax.axis_index(a) for a in AXES)
    start_row = lax.axis_index(AXES) * rows
    positions = start_row + jnp.arange(rows, dtype=jnp.int32)

    angles = positions.astype(jnp.float32)[:, None] * jnp.tile(frequencies(width), 2)[None, :]
    cosine = jnp.cos(angles)
    signed_sine = jnp.sin(angles) * jnp.where(jnp.arange(width) < width // 2, -1.0, 1.0)

    pair = prepare_pair(keys, values, cosine, signed_sine)
    pair = lax.all_to_all(pair, ("yl", "sy"), split_axis=0, concat_axis=0, tiled=True)
    pair = pair.swapaxes(0, 1).reshape(2, 2, -1, width)
    block = pair.shape[2]
    own_values = pair[1].reshape(2, block // 128, 128, width).swapaxes(2, 3).reshape(2, block, width)
    c = jnp.concatenate([pair[0], own_values], axis=1)
    ahead = [(i, (i + 1) % 4) for i in range(4)]
    behind = [(i, (i - 1) % 4) for i in range(4)]
    swap = [(0, 1), (1, 0)]
    u = lax.ppermute(c, "x", ahead)
    v = lax.ppermute(c, "x", behind)
    near = []
    for piece in (c, u, v):
        near += [piece, lax.ppermute(piece, "core", swap)]
    far = []
    for source, half, way in ((near[2], 0, ahead), (near[4], 1, behind), (near[3], 0, ahead), (near[5], 1, behind)):
        far.append(lax.ppermute(source[half:half + 1], "x", way))
    pieces = near + [far[0], far[2], far[1], far[3]]
    where = jnp.stack([x, core]).astype(jnp.int32)

    ordered = prepare_queries(queries, cosine, signed_sine, group)
    arrived = []
    for n in range(CHUNKS):
        arrived.append(lax.all_to_all(ordered[n], AXES, split_axis=0, concat_axis=0, tiled=True))
    halves = []
    for n in range(CHUNKS):
        done = attn(arrived[n], pieces, where, bq=TILE, period=rows, which=n)
        back = lax.all_to_all(done, AXES, split_axis=0, concat_axis=0, tiled=True)
        back = back.reshape(group, key_heads, -1, width).transpose(2, 1, 0, 3)
        halves.append(back.reshape(-1, heads_all, width))
    whole = lax.optimization_barrier(jnp.pad(halves[0], ((0, rows - rows // CHUNKS), (0, 0), (0, 0))))
    for n in range(1, CHUNKS):
        whole = lax.dynamic_update_slice(whole, halves[n], (n * (rows // CHUNKS), 0, 0))
    return whole


def solution(mesh):
    finer = Mesh(mesh.devices.reshape(4, 2, 2, 8), AXES)
    placed = P(AXES, None, None)

    return jax.shard_map(shards, mesh=finer, in_specs=(placed,) * 3, out_specs=placed, check_vma=False)
```

```python
import math

import jax
import jax.numpy as jnp
from jax import lax
from jax.experimental import pallas as pl
from jax.experimental.pallas import tpu as pltpu
from jax.sharding import Mesh, PartitionSpec as P


LOG2E = 1.4426950408889634
LOW, HIGH = 2.0**-80, 2.0**100
CHUNKS = 2
TILE = 2048
GROUPS = {8: {0: (0,), 1: tuple(range(1, 8))}}
AXES = ("x", "yl", "core", "sy")


def frequencies(head_width):
    half_index = jnp.arange(head_width // 2, dtype=jnp.float32)
    base_rate = jnp.power(jnp.float32(500000.0), -2.0 * half_index / head_width)
    wavelen = 2.0 * math.pi / base_rate
    smooth = (8192.0 / wavelen - 1.0) / 3.0
    blended = (1.0 - smooth) * base_rate / 8.0 + smooth * base_rate
    return jnp.where(
        wavelen < 2048.0, base_rate, jnp.where(wavelen > 8192.0, base_rate / 8.0, blended)
    )


def doubled(cos_ref, sin_ref):
    cosine, sine = cos_ref[...], sin_ref[...]
    return jnp.concatenate([cosine, cosine], axis=1), jnp.concatenate([-sine, sine], axis=1)


def turned(head, cosine, signed_sine):
    return head * cosine + pltpu.roll(head, head.shape[-1] // 2, 1) * signed_sine


def prepare_pair(keys, values, cosine, sine):
    rows, heads, width = keys.shape

    def kernel(k_ref, v_ref, cos_ref, sin_ref, o_ref, kf_ref, vf_ref):
        tables = doubled(cos_ref, sin_ref)
        kf_ref[...] = k_ref[...].astype(jnp.float32)
        vf_ref[...] = v_ref[...].astype(jnp.float32)
        for h in range(heads):
            key = turned(kf_ref[:, h, :], *tables).astype(jnp.bfloat16)
            value = vf_ref[:, h, :].astype(jnp.bfloat16)
            for half in (0, heads):
                o_ref[half + h, 0] = key
                o_ref[half + h, 1] = value

    wide = pltpu.VMEM((rows, heads, width), jnp.float32)
    return pl.pallas_call(
        kernel, out_shape=jax.ShapeDtypeStruct((2 * heads, 2, rows, width), jnp.bfloat16),
        scratch_shapes=[wide, wide], name="pair",
    )(keys, values, cosine, sine)


def prepare_queries(queries, cosine, sine, group):
    rows, heads, width = queries.shape
    strip = rows // CHUNKS

    def kernel(q_ref, cos_ref, sin_ref, *rest):
        outs, wide_ref = rest[:-1], rest[-1]
        tables = doubled(cos_ref, sin_ref)
        wide_ref[...] = q_ref[...].astype(jnp.float32)
        for h in range(group):
            head = turned(wide_ref[:, h, :], *tables).astype(jnp.bfloat16)
            for n, o_ref in enumerate(outs):
                o_ref[h, 0] = head[n * strip:(n + 1) * strip]

    table = pl.BlockSpec((rows, width // 2), lambda g: (0, 0))
    parts = pl.pallas_call(
        kernel, grid=(heads // group,),
        in_specs=[pl.BlockSpec((rows, group, width), lambda g: (0, g, 0)), table, table],
        out_specs=[pl.BlockSpec((group, 1, strip, width), lambda g: (0, g, 0, 0))] * CHUNKS,
        out_shape=[jax.ShapeDtypeStruct((group, heads // group, strip, width), jnp.bfloat16)] * CHUNKS,
        scratch_shapes=[pltpu.VMEM((rows, group, width), jnp.float32)], name="queries",
    )(queries, cosine, sine)
    return [part.reshape(heads, strip, width) for part in parts]


def attn(q, pieces, where, *, bq, period, which, sub=512, unroll=4):
    G, strip, D = q.shape
    BK = pieces[0].shape[1] // 2
    blocks = G * period // BK
    c = LOG2E / math.sqrt(D)
    devs = bq // strip
    nd = devs * period // BK
    w = bq // nd
    offset = which * strip
    groups = GROUPS[nd]

    def kernel(where_ref, q_ref, c_ref, cc_ref, u_ref, cu_ref, v_ref, cv_ref, h_ref, ch_ref, g_ref, cg_ref,
               *rest):
        o_ref, qT_ref, acc_ref, l_ref, kv_ref, qv_ref, sems = rest[-7:]
        qi = pl.program_id(0)
        first = qi * nd

        @pl.when(qi == 0)
        def _():
            pltpu.make_async_copy(q_ref, qv_ref, sems.at[blocks]).start()
            x, core = where_ref[0], where_ref[1]
            for plane in range(4):
                for step, refs in ((0, (c_ref, cc_ref)), (3, (u_ref, cu_ref)), (1, (v_ref, cv_ref)),
                                   (2, ((h_ref, g_ref), (ch_ref, cg_ref)))):
                    @pl.when(lax.rem(x + step, 4) == plane)
                    def _():
                        for yl in (0, 1):
                            for other in (0, 1):
                                src = refs[other][yl].at[0] if step == 2 else refs[other].at[yl]
                                b = plane * 4 + yl * 2 + lax.rem(core + other, 2)
                                pltpu.make_async_copy(src, kv_ref.at[b], sems.at[b]).start()

        @pl.when(qi == 0)
        def _():
            pltpu.make_async_copy(q_ref, qv_ref, sems.at[blocks]).wait()

        def landed(t):
            pltpu.make_async_copy(c_ref.at[0], kv_ref.at[first + t], sems.at[first + t]).wait()


        def values(blk, lo, n):
            return jnp.concatenate(
                [kv_ref[blk, BK + lo + t * 128: BK + lo + (t + 1) * 128, :] for t in range(n // 128)], axis=1)

        def block(blk, lo, masked, fresh=False):
            for s in range(0, BK, sub):
                k = kv_ref[blk, s:s + sub, :]
                rows = qv_ref[pl.ds(qi * devs + lo // strip, devs - lo // strip)].reshape(bq - lo, D)
                st = lax.dot_general(k, rows, (((1,), (1,)), ((), ())), preferred_element_type=jnp.float32)
                p = jnp.exp2(st * c)
                if masked:
                    lane = lax.broadcasted_iota(jnp.int32, (1, w), 1)
                    at = lane // strip * period + offset + lane % strip
                    row = s + lax.broadcasted_iota(jnp.int32, (sub, 1), 0)
                    head = jnp.where(row <= at, p[:, :w], 0.0)
                    p = jnp.concatenate([head, p[:, w:]], axis=1) if bq - lo > w else head
                mass = jnp.sum(p.reshape(sub // 8, 8, bq - lo), axis=0)
                mixed = jnp.dot(values(blk, s, sub), p.astype(jnp.bfloat16), preferred_element_type=jnp.float32)
                if fresh:
                    l_ref[:, lo:] = mass
                    acc_ref[:, lo:] = mixed
                else:
                    l_ref[:, lo:] += mass
                    acc_ref[:, lo:] += mixed

        def body(j, _):
            for u in range(unroll):
                block(j * unroll + u, 0, False)
            return 0

        for t in range(nd):
            for later in groups.get(t, ()):
                landed(later)
            block(first + t, t * w, True, t == 0)
        lax.fori_loop(0, first // unroll, body, 0)
        total = jnp.sum(l_ref[...], axis=0, keepdims=True)
        o_ref[...] = (acc_ref[...] * (1.0 / total)).T.astype(jnp.bfloat16).reshape(o_ref.shape)
        fine = jnp.logical_and(jnp.min(total) > LOW, jnp.max(total) < HIGH)

        @pl.when(jnp.logical_not(fine))
        def _():
            qT_ref[...] = qv_ref[pl.ds(qi * devs, devs)].reshape(bq, D).astype(jnp.float32).T.astype(jnp.bfloat16)
            lane = lax.broadcasted_iota(jnp.int32, (1, bq), 1)
            at = qi * devs * period + lane // strip * period + offset + lane % strip

            def slow(blk, state):
                l, m = state
                st = jnp.dot(kv_ref[blk, :BK, :], qT_ref[...], preferred_element_type=jnp.float32) * c
                row = blk * BK + lax.broadcasted_iota(jnp.int32, (BK, 1), 0)
                st = jnp.where(row <= at, st, -jnp.inf)
                top = jnp.maximum(m, jnp.max(st, axis=0, keepdims=True))
                shrink = jnp.exp2(m - top)
                p = jnp.exp2(st - top)
                acc_ref[...] = acc_ref[...] * shrink + jnp.dot(
                    values(blk, 0, BK), p.astype(jnp.bfloat16), preferred_element_type=jnp.float32)
                return l * shrink + jnp.sum(p, axis=0, keepdims=True), top

            acc_ref[...] = jnp.zeros_like(acc_ref)
            start = (jnp.zeros((1, bq), jnp.float32), jnp.full((1, bq), -1e30, jnp.float32))
            l, _ = lax.fori_loop(0, first + nd, slow, start)
            o_ref[...] = (acc_ref[...] / l).T.astype(jnp.bfloat16).reshape(o_ref.shape)

    anywhere = pl.BlockSpec(memory_space=pl.ANY)
    return pl.pallas_call(
        kernel, grid=(G // devs,),
        in_specs=[pl.BlockSpec(memory_space=pltpu.SMEM),
                  anywhere] + [anywhere] * len(pieces),
        out_specs=pl.BlockSpec((devs, strip, D), lambda i: (i, 0, 0)),
        out_shape=jax.ShapeDtypeStruct((G, strip, D), jnp.bfloat16),
        scratch_shapes=[pltpu.VMEM((D, bq), jnp.bfloat16), pltpu.VMEM((D, bq), jnp.float32),
                        pltpu.VMEM((8, bq), jnp.float32), pltpu.VMEM((blocks, 2 * BK, D), jnp.bfloat16),
                        pltpu.VMEM((G, strip, D), jnp.bfloat16),
                        pltpu.SemaphoreType.DMA((blocks + 1,))],
        compiler_params=pltpu.CompilerParams(vmem_limit_bytes=24 * 2**20),
        name="attn",
    )(where, *(pltpu.with_memory_space_constraint(piece, pltpu.HBM) for piece in (q, *pieces)))


def shards(queries, keys, values):
    rows, heads_all, width = queries.shape
    key_heads = keys.shape[1]
    group = heads_all // key_heads
    x, _, core, _ = (lax.axis_index(a) for a in AXES)
    start_row = lax.axis_index(AXES) * rows
    positions = start_row + jnp.arange(rows, dtype=jnp.int32)

    angles = positions.astype(jnp.float32)[:, None] * frequencies(width)[None, :]
    cosine, sine = jnp.cos(angles), jnp.sin(angles)

    pair = prepare_pair(keys, values, cosine, sine)
    pair = lax.all_to_all(pair, ("yl", "sy"), split_axis=0, concat_axis=0, tiled=True)
    pair = pair.swapaxes(0, 1).reshape(2, 2, -1, width)
    block = pair.shape[2]
    own_values = pair[1].reshape(2, block // 128, 128, width).swapaxes(2, 3).reshape(2, block, width)
    c = jnp.concatenate([pair[0], own_values], axis=1)
    ahead = [(i, (i + 1) % 4) for i in range(4)]
    behind = [(i, (i - 1) % 4) for i in range(4)]
    swap = [(0, 1), (1, 0)]
    u = lax.ppermute(c, "x", ahead)
    v = lax.ppermute(c, "x", behind)
    near = []
    for piece in (c, u, v):
        near += [piece, lax.ppermute(piece, "core", swap)]
    far = []
    for source, half, way in ((near[2], 0, ahead), (near[4], 1, behind), (near[3], 0, ahead), (near[5], 1, behind)):
        far.append(lax.ppermute(source[half:half + 1], "x", way))
    pieces = near + [far[0], far[2], far[1], far[3]]
    where = jnp.stack([x, core]).astype(jnp.int32)

    ordered = prepare_queries(queries, cosine, sine, group)
    arrived = []
    for n in range(CHUNKS):
        arrived.append(lax.all_to_all(ordered[n], AXES, split_axis=0, concat_axis=0, tiled=True))
    halves = []
    for n in range(CHUNKS):
        done = attn(arrived[n], pieces, where, bq=TILE, period=rows, which=n)
        back = lax.all_to_all(done, AXES, split_axis=0, concat_axis=0, tiled=True)
        back = back.reshape(group, key_heads, -1, width).transpose(2, 1, 0, 3)
        halves.append(back.reshape(-1, heads_all, width))
    whole = lax.optimization_barrier(jnp.pad(halves[0], ((0, rows - rows // CHUNKS), (0, 0), (0, 0))))
    for n in range(1, CHUNKS):
        whole = lax.dynamic_update_slice(whole, halves[n], (n * (rows // CHUNKS), 0, 0))
    return whole


def solution(mesh):
    finer = Mesh(mesh.devices.reshape(4, 2, 2, 8), AXES)
    placed = P(AXES, None, None)

    return jax.shard_map(shards, mesh=finer, in_specs=(placed,) * 3, out_specs=placed, check_vma=False)
```

```python
import math

import jax
import jax.numpy as jnp
from jax import lax
from jax.experimental import pallas as pl
from jax.experimental.pallas import tpu as pltpu
from jax.sharding import Mesh, PartitionSpec as P


LOG2E = 1.4426950408889634
LOW, HIGH = 2.0**-80, 2.0**100
CHUNKS = 2
TILE = 2048
GROUPS = {8: {0: (0,), 1: tuple(range(1, 8))}}
AXES = ("x", "yl", "core", "sy")


def frequencies(head_width):
    half_index = jnp.arange(head_width // 2, dtype=jnp.float32)
    base_rate = jnp.power(jnp.float32(500000.0), -2.0 * half_index / head_width)
    wavelen = 2.0 * math.pi / base_rate
    smooth = (8192.0 / wavelen - 1.0) / 3.0
    blended = (1.0 - smooth) * base_rate / 8.0 + smooth * base_rate
    return jnp.where(
        wavelen < 2048.0, base_rate, jnp.where(wavelen > 8192.0, base_rate / 8.0, blended)
    )


def turned(head, cosine, signed_sine):
    return head * cosine + pltpu.roll(head, head.shape[-1] // 2, 1) * signed_sine


def prepare_pair(keys, values, cosine, signed_sine):
    rows, heads, width = keys.shape

    def kernel(k_ref, v_ref, cos_ref, sin_ref, o_ref, kf_ref, vf_ref):
        kf_ref[...] = k_ref[...].astype(jnp.float32)
        vf_ref[...] = v_ref[...].astype(jnp.float32)
        for h in range(heads):
            key = turned(kf_ref[:, h, :], cos_ref[...], sin_ref[...]).astype(jnp.bfloat16)
            value = vf_ref[:, h, :].astype(jnp.bfloat16)
            for half in (0, heads):
                o_ref[half + h, 0] = key
                o_ref[half + h, 1] = value

    wide = pltpu.VMEM((rows, heads, width), jnp.float32)
    return pl.pallas_call(
        kernel, out_shape=jax.ShapeDtypeStruct((2 * heads, 2, rows, width), jnp.bfloat16),
        scratch_shapes=[wide, wide], name="pair",
        compiler_params=pltpu.CompilerParams(vmem_limit_bytes=16 * 2**20),
    )(*(pltpu.with_memory_space_constraint(a, pltpu.HBM) for a in (keys, values)), cosine, signed_sine)


def prepare_queries(queries, cosine, signed_sine, group):
    rows, heads, width = queries.shape
    strip = rows // CHUNKS

    def kernel(q_ref, cos_ref, sin_ref, *rest):
        outs, wide_ref = rest[:-1], rest[-1]
        wide_ref[...] = q_ref[...].astype(jnp.float32)
        for h in range(group):
            head = turned(wide_ref[:, h, :], cos_ref[...], sin_ref[...]).astype(jnp.bfloat16)
            for n, o_ref in enumerate(outs):
                o_ref[h, 0] = head[n * strip:(n + 1) * strip]

    table = pl.BlockSpec((rows, width), lambda g: (0, 0))
    parts = pl.pallas_call(
        kernel, grid=(heads // group,),
        in_specs=[pl.BlockSpec((rows, group, width), lambda g: (0, g, 0)), table, table],
        out_specs=[pl.BlockSpec((group, 1, strip, width), lambda g: (0, g, 0, 0))] * CHUNKS,
        out_shape=[jax.ShapeDtypeStruct((group, heads // group, strip, width), jnp.bfloat16)] * CHUNKS,
        scratch_shapes=[pltpu.VMEM((rows, group, width), jnp.float32)], name="queries",
    )(queries, cosine, signed_sine)
    return [part.reshape(heads, strip, width) for part in parts]


def attn(q, pieces, where, *, bq, period, which, sub=512, unroll=4):
    G, strip, D = q.shape
    BK = pieces[0].shape[1] // 2
    blocks = G * period // BK
    c = LOG2E / math.sqrt(D)
    devs = bq // strip
    nd = devs * period // BK
    tiles = G // devs
    w = bq // nd
    offset = which * strip
    groups = GROUPS[nd]

    def kernel(where_ref, q_ref, c_ref, cc_ref, u_ref, cu_ref, v_ref, cv_ref, h_ref, ch_ref, g_ref, cg_ref,
               *rest):
        o_ref, qT_ref, acc_ref, l_ref, kv_ref, qv_ref, sems = rest[-7:]
        qi = pl.program_id(0)
        first = qi * nd

        def queries_in(n):
            part = pl.ds(n * devs, devs)
            return pltpu.make_async_copy(q_ref.at[part], qv_ref.at[part], sems.at[blocks + n])

        @pl.when(qi == 0)
        def _():
            queries_in(0).start()
            x, core = where_ref[0], where_ref[1]
            for plane in range(4):
                for step, refs in ((0, (c_ref, cc_ref)), (3, (u_ref, cu_ref)), (1, (v_ref, cv_ref)),
                                   (2, ((h_ref, g_ref), (ch_ref, cg_ref)))):
                    @pl.when(lax.rem(x + step, 4) == plane)
                    def _():
                        for yl in (0, 1):
                            for other in (0, 1):
                                src = refs[other][yl].at[0] if step == 2 else refs[other].at[yl]
                                b = plane * 4 + yl * 2 + lax.rem(core + other, 2)
                                pltpu.make_async_copy(src, kv_ref.at[b], sems.at[b]).start()

            for n in range(1, tiles):
                queries_in(n).start()

        queries_in(qi).wait()

        def landed(t):
            pltpu.make_async_copy(c_ref.at[0], kv_ref.at[first + t], sems.at[first + t]).wait()


        def values(blk, lo, n):
            return jnp.concatenate(
                [kv_ref[blk, BK + lo + t * 128: BK + lo + (t + 1) * 128, :] for t in range(n // 128)], axis=1)

        def block(blk, lo, masked, fresh=False):
            for s in range(0, BK, sub):
                k = kv_ref[blk, s:s + sub, :]
                rows = qv_ref[pl.ds(qi * devs + lo // strip, devs - lo // strip)].reshape(bq - lo, D)
                st = lax.dot_general(k, rows, (((1,), (1,)), ((), ())), preferred_element_type=jnp.float32)
                p = jnp.exp2(st * c)
                if masked:
                    lane = lax.broadcasted_iota(jnp.int32, (1, w), 1)
                    at = lane // strip * period + offset + lane % strip
                    row = s + lax.broadcasted_iota(jnp.int32, (sub, 1), 0)
                    head = jnp.where(row <= at, p[:, :w], 0.0)
                    p = jnp.concatenate([head, p[:, w:]], axis=1) if bq - lo > w else head
                mass = jnp.sum(p.reshape(sub // 8, 8, bq - lo), axis=0)
                mixed = jnp.dot(values(blk, s, sub), p.astype(jnp.bfloat16), preferred_element_type=jnp.float32)
                if fresh:
                    l_ref[:, lo:] = mass
                    acc_ref[:, lo:] = mixed
                else:
                    l_ref[:, lo:] += mass
                    acc_ref[:, lo:] += mixed

        def body(j, _):
            for u in range(unroll):
                block(j * unroll + u, 0, False)
            return 0

        for t in range(nd):
            for later in groups.get(t, ()):
                landed(later)
            block(first + t, t * w, True, t == 0)
        lax.fori_loop(0, first // unroll, body, 0)
        total = jnp.sum(l_ref[...], axis=0, keepdims=True)
        o_ref[...] = (acc_ref[...] * (1.0 / total)).T.astype(jnp.bfloat16).reshape(o_ref.shape)
        fine = jnp.logical_and(jnp.min(total) > LOW, jnp.max(total) < HIGH)

        @pl.when(jnp.logical_not(fine))
        def _():
            qT_ref[...] = qv_ref[pl.ds(qi * devs, devs)].reshape(bq, D).astype(jnp.float32).T.astype(jnp.bfloat16)
            lane = lax.broadcasted_iota(jnp.int32, (1, bq), 1)
            at = qi * devs * period + lane // strip * period + offset + lane % strip

            def slow(blk, state):
                l, m = state
                st = jnp.dot(kv_ref[blk, :BK, :], qT_ref[...], preferred_element_type=jnp.float32) * c
                row = blk * BK + lax.broadcasted_iota(jnp.int32, (BK, 1), 0)
                st = jnp.where(row <= at, st, -jnp.inf)
                top = jnp.maximum(m, jnp.max(st, axis=0, keepdims=True))
                shrink = jnp.exp2(m - top)
                p = jnp.exp2(st - top)
                acc_ref[...] = acc_ref[...] * shrink + jnp.dot(
                    values(blk, 0, BK), p.astype(jnp.bfloat16), preferred_element_type=jnp.float32)
                return l * shrink + jnp.sum(p, axis=0, keepdims=True), top

            acc_ref[...] = jnp.zeros_like(acc_ref)
            start = (jnp.zeros((1, bq), jnp.float32), jnp.full((1, bq), -1e30, jnp.float32))
            l, _ = lax.fori_loop(0, first + nd, slow, start)
            o_ref[...] = (acc_ref[...] / l).T.astype(jnp.bfloat16).reshape(o_ref.shape)

    anywhere = pl.BlockSpec(memory_space=pl.ANY)
    return pl.pallas_call(
        kernel, grid=(G // devs,),
        in_specs=[pl.BlockSpec(memory_space=pltpu.SMEM),
                  anywhere] + [anywhere] * len(pieces),
        out_specs=pl.BlockSpec((devs, strip, D), lambda i: (i, 0, 0)),
        out_shape=jax.ShapeDtypeStruct((G, strip, D), jnp.bfloat16),
        scratch_shapes=[pltpu.VMEM((D, bq), jnp.bfloat16), pltpu.VMEM((D, bq), jnp.float32),
                        pltpu.VMEM((8, bq), jnp.float32), pltpu.VMEM((blocks, 2 * BK, D), jnp.bfloat16),
                        pltpu.VMEM((G, strip, D), jnp.bfloat16),
                        pltpu.SemaphoreType.DMA((blocks + tiles,))],
        compiler_params=pltpu.CompilerParams(vmem_limit_bytes=24 * 2**20),
        name="attn",
    )(where, *(pltpu.with_memory_space_constraint(piece, pltpu.HBM) for piece in (q, *pieces)))


def shards(queries, keys, values):
    rows, heads_all, width = queries.shape
    key_heads = keys.shape[1]
    group = heads_all // key_heads
    x, _, core, _ = (lax.axis_index(a) for a in AXES)
    start_row = lax.axis_index(AXES) * rows
    positions = start_row + jnp.arange(rows, dtype=jnp.int32)

    angles = positions.astype(jnp.float32)[:, None] * jnp.tile(frequencies(width), 2)[None, :]
    cosine = jnp.cos(angles)
    signed_sine = jnp.sin(angles) * jnp.where(jnp.arange(width) < width // 2, -1.0, 1.0)

    pair = prepare_pair(keys, values, cosine, signed_sine)
    pair = lax.all_to_all(pair, ("yl", "sy"), split_axis=0, concat_axis=0, tiled=True)
    pair = pair.swapaxes(0, 1).reshape(2, 2, -1, width)
    block = pair.shape[2]
    own_values = pair[1].reshape(2, block // 128, 128, width).swapaxes(2, 3).reshape(2, block, width)
    c = jnp.concatenate([pair[0], own_values], axis=1)
    ahead = [(i, (i + 1) % 4) for i in range(4)]
    behind = [(i, (i - 1) % 4) for i in range(4)]
    swap = [(0, 1), (1, 0)]
    u = lax.ppermute(c, "x", ahead)
    v = lax.ppermute(c, "x", behind)
    near = []
    for piece in (c, u, v):
        near += [piece, lax.ppermute(piece, "core", swap)]
    far = []
    for source, half, way in ((near[2], 0, ahead), (near[4], 1, behind), (near[3], 0, ahead), (near[5], 1, behind)):
        far.append(lax.ppermute(source[half:half + 1], "x", way))
    pieces = near + [far[0], far[2], far[1], far[3]]
    where = jnp.stack([x, core]).astype(jnp.int32)

    ordered = prepare_queries(queries, cosine, signed_sine, group)
    arrived = []
    for n in range(CHUNKS):
        arrived.append(lax.all_to_all(ordered[n], AXES, split_axis=0, concat_axis=0, tiled=True))
    halves = []
    for n in range(CHUNKS):
        done = attn(arrived[n], pieces, where, bq=TILE, period=rows, which=n)
        back = lax.all_to_all(done, AXES, split_axis=0, concat_axis=0, tiled=True)
        back = back.reshape(group, key_heads, -1, width).transpose(2, 1, 0, 3)
        halves.append(back.reshape(-1, heads_all, width))
    whole = lax.optimization_barrier(jnp.pad(halves[0], ((0, rows - rows // CHUNKS), (0, 0), (0, 0))))
    for n in range(1, CHUNKS):
        whole = lax.dynamic_update_slice(whole, halves[n], (n * (rows // CHUNKS), 0, 0))
    return whole


def solution(mesh):
    finer = Mesh(mesh.devices.reshape(4, 2, 2, 8), AXES)
    placed = P(AXES, None, None)

    return jax.shard_map(shards, mesh=finer, in_specs=(placed,) * 3, out_specs=placed, check_vma=False)
```

```python
import math

import jax
import jax.numpy as jnp
from jax import lax
from jax.experimental import pallas as pl
from jax.experimental.pallas import tpu as pltpu
from jax.sharding import Mesh, PartitionSpec as P


LOG2E = 1.4426950408889634
LOW, HIGH = 2.0**-80, 2.0**100
CHUNKS = 2
TILE = 2048
GROUPS = {8: {0: (0,), 1: tuple(range(1, 8))}}
AXES = ("x", "yl", "core", "sy")


def frequencies(head_width):
    half_index = jnp.arange(head_width // 2, dtype=jnp.float32)
    base_rate = jnp.power(jnp.float32(500000.0), -2.0 * half_index / head_width)
    wavelen = 2.0 * math.pi / base_rate
    smooth = (8192.0 / wavelen - 1.0) / 3.0
    blended = (1.0 - smooth) * base_rate / 8.0 + smooth * base_rate
    return jnp.where(
        wavelen < 2048.0, base_rate, jnp.where(wavelen > 8192.0, base_rate / 8.0, blended)
    )


def doubled(cos_ref, sin_ref):
    cosine, sine = cos_ref[...], sin_ref[...]
    return jnp.concatenate([cosine, cosine], axis=1), jnp.concatenate([-sine, sine], axis=1)


def turned(head, cosine, signed_sine):
    return head * cosine + pltpu.roll(head, head.shape[-1] // 2, 1) * signed_sine


def prepare_pair(keys, values, cosine, sine):
    rows, heads, width = keys.shape

    def kernel(k_ref, v_ref, cos_ref, sin_ref, o_ref, kf_ref, vf_ref):
        tables = doubled(cos_ref, sin_ref)
        kf_ref[...] = k_ref[...].astype(jnp.float32)
        vf_ref[...] = v_ref[...].astype(jnp.float32)
        for h in range(heads):
            key = turned(kf_ref[:, h, :], *tables).astype(jnp.bfloat16)
            value = vf_ref[:, h, :].astype(jnp.bfloat16)
            for half in (0, heads):
                o_ref[half + h, 0] = key
                o_ref[half + h, 1] = value

    wide = pltpu.VMEM((rows, heads, width), jnp.float32)
    return pl.pallas_call(
        kernel, out_shape=jax.ShapeDtypeStruct((2 * heads, 2, rows, width), jnp.bfloat16),
        scratch_shapes=[wide, wide], name="pair",
        compiler_params=pltpu.CompilerParams(vmem_limit_bytes=16 * 2**20),
    )(*(pltpu.with_memory_space_constraint(a, pltpu.HBM) for a in (keys, values)), cosine, sine)


def prepare_queries(queries, cosine, sine, group):
    rows, heads, width = queries.shape
    strip = rows // CHUNKS

    def kernel(q_ref, cos_ref, sin_ref, *rest):
        outs, wide_ref = rest[:-1], rest[-1]
        tables = doubled(cos_ref, sin_ref)
        wide_ref[...] = q_ref[...].astype(jnp.float32)
        for h in range(group):
            head = turned(wide_ref[:, h, :], *tables).astype(jnp.bfloat16)
            for n, o_ref in enumerate(outs):
                o_ref[h, 0] = head[n * strip:(n + 1) * strip]

    table = pl.BlockSpec((rows, width // 2), lambda g: (0, 0))
    parts = pl.pallas_call(
        kernel, grid=(heads // group,),
        in_specs=[pl.BlockSpec((rows, group, width), lambda g: (0, g, 0)), table, table],
        out_specs=[pl.BlockSpec((group, 1, strip, width), lambda g: (0, g, 0, 0))] * CHUNKS,
        out_shape=[jax.ShapeDtypeStruct((group, heads // group, strip, width), jnp.bfloat16)] * CHUNKS,
        scratch_shapes=[pltpu.VMEM((rows, group, width), jnp.float32)], name="queries",
    )(queries, cosine, sine)
    return [part.reshape(heads, strip, width) for part in parts]


def attn(q, pieces, where, *, bq, period, which, sub=512, unroll=4):
    G, strip, D = q.shape
    BK = pieces[0].shape[1] // 2
    blocks = G * period // BK
    c = LOG2E / math.sqrt(D)
    devs = bq // strip
    nd = devs * period // BK
    tiles = G // devs
    w = bq // nd
    offset = which * strip
    groups = GROUPS[nd]

    def kernel(where_ref, q_ref, c_ref, cc_ref, u_ref, cu_ref, v_ref, cv_ref, h_ref, ch_ref, g_ref, cg_ref,
               *rest):
        o_ref, qT_ref, acc_ref, l_ref, kv_ref, qv_ref, sems = rest[-7:]
        qi = pl.program_id(0)
        first = qi * nd

        def queries_in(n):
            part = pl.ds(n * devs, devs)
            return pltpu.make_async_copy(q_ref.at[part], qv_ref.at[part], sems.at[blocks + n])

        @pl.when(qi == 0)
        def _():
            queries_in(0).start()
            x, core = where_ref[0], where_ref[1]
            for plane in range(4):
                for step, refs in ((0, (c_ref, cc_ref)), (3, (u_ref, cu_ref)), (1, (v_ref, cv_ref)),
                                   (2, ((h_ref, g_ref), (ch_ref, cg_ref)))):
                    @pl.when(lax.rem(x + step, 4) == plane)
                    def _():
                        for yl in (0, 1):
                            for other in (0, 1):
                                src = refs[other][yl].at[0] if step == 2 else refs[other].at[yl]
                                b = plane * 4 + yl * 2 + lax.rem(core + other, 2)
                                pltpu.make_async_copy(src, kv_ref.at[b], sems.at[b]).start()

            for n in range(1, tiles):
                queries_in(n).start()

        queries_in(qi).wait()

        def landed(t):
            pltpu.make_async_copy(c_ref.at[0], kv_ref.at[first + t], sems.at[first + t]).wait()


        def values(blk, lo, n):
            return jnp.concatenate(
                [kv_ref[blk, BK + lo + t * 128: BK + lo + (t + 1) * 128, :] for t in range(n // 128)], axis=1)

        def block(blk, lo, masked, fresh=False):
            for s in range(0, BK, sub):
                k = kv_ref[blk, s:s + sub, :]
                rows = qv_ref[pl.ds(qi * devs + lo // strip, devs - lo // strip)].reshape(bq - lo, D)
                st = lax.dot_general(k, rows, (((1,), (1,)), ((), ())), preferred_element_type=jnp.float32)
                p = jnp.exp2(st * c)
                if masked:
                    lane = lax.broadcasted_iota(jnp.int32, (1, w), 1)
                    at = lane // strip * period + offset + lane % strip
                    row = s + lax.broadcasted_iota(jnp.int32, (sub, 1), 0)
                    head = jnp.where(row <= at, p[:, :w], 0.0)
                    p = jnp.concatenate([head, p[:, w:]], axis=1) if bq - lo > w else head
                mass = jnp.sum(p.reshape(sub // 8, 8, bq - lo), axis=0)
                mixed = jnp.dot(values(blk, s, sub), p.astype(jnp.bfloat16), preferred_element_type=jnp.float32)
                if fresh:
                    l_ref[:, lo:] = mass
                    acc_ref[:, lo:] = mixed
                else:
                    l_ref[:, lo:] += mass
                    acc_ref[:, lo:] += mixed

        def body(j, _):
            for u in range(unroll):
                block(j * unroll + u, 0, False)
            return 0

        for t in range(nd):
            for later in groups.get(t, ()):
                landed(later)
            block(first + t, t * w, True, t == 0)
        lax.fori_loop(0, first // unroll, body, 0)
        total = jnp.sum(l_ref[...], axis=0, keepdims=True)
        o_ref[...] = (acc_ref[...] * (1.0 / total)).T.astype(jnp.bfloat16).reshape(o_ref.shape)
        fine = jnp.logical_and(jnp.min(total) > LOW, jnp.max(total) < HIGH)

        @pl.when(jnp.logical_not(fine))
        def _():
            qT_ref[...] = qv_ref[pl.ds(qi * devs, devs)].reshape(bq, D).astype(jnp.float32).T.astype(jnp.bfloat16)
            lane = lax.broadcasted_iota(jnp.int32, (1, bq), 1)
            at = qi * devs * period + lane // strip * period + offset + lane % strip

            def slow(blk, state):
                l, m = state
                st = jnp.dot(kv_ref[blk, :BK, :], qT_ref[...], preferred_element_type=jnp.float32) * c
                row = blk * BK + lax.broadcasted_iota(jnp.int32, (BK, 1), 0)
                st = jnp.where(row <= at, st, -jnp.inf)
                top = jnp.maximum(m, jnp.max(st, axis=0, keepdims=True))
                shrink = jnp.exp2(m - top)
                p = jnp.exp2(st - top)
                acc_ref[...] = acc_ref[...] * shrink + jnp.dot(
                    values(blk, 0, BK), p.astype(jnp.bfloat16), preferred_element_type=jnp.float32)
                return l * shrink + jnp.sum(p, axis=0, keepdims=True), top

            acc_ref[...] = jnp.zeros_like(acc_ref)
            start = (jnp.zeros((1, bq), jnp.float32), jnp.full((1, bq), -1e30, jnp.float32))
            l, _ = lax.fori_loop(0, first + nd, slow, start)
            o_ref[...] = (acc_ref[...] / l).T.astype(jnp.bfloat16).reshape(o_ref.shape)

    anywhere = pl.BlockSpec(memory_space=pl.ANY)
    return pl.pallas_call(
        kernel, grid=(G // devs,),
        in_specs=[pl.BlockSpec(memory_space=pltpu.SMEM),
                  anywhere] + [anywhere] * len(pieces),
        out_specs=pl.BlockSpec((devs, strip, D), lambda i: (i, 0, 0)),
        out_shape=jax.ShapeDtypeStruct((G, strip, D), jnp.bfloat16),
        scratch_shapes=[pltpu.VMEM((D, bq), jnp.bfloat16), pltpu.VMEM((D, bq), jnp.float32),
                        pltpu.VMEM((8, bq), jnp.float32), pltpu.VMEM((blocks, 2 * BK, D), jnp.bfloat16),
                        pltpu.VMEM((G, strip, D), jnp.bfloat16),
                        pltpu.SemaphoreType.DMA((blocks + tiles,))],
        compiler_params=pltpu.CompilerParams(vmem_limit_bytes=24 * 2**20),
        name="attn",
    )(where, *(pltpu.with_memory_space_constraint(piece, pltpu.HBM) for piece in (q, *pieces)))


def shards(queries, keys, values):
    rows, heads_all, width = queries.shape
    key_heads = keys.shape[1]
    group = heads_all // key_heads
    x, _, core, _ = (lax.axis_index(a) for a in AXES)
    start_row = lax.axis_index(AXES) * rows
    positions = start_row + jnp.arange(rows, dtype=jnp.int32)

    angles = positions.astype(jnp.float32)[:, None] * frequencies(width)[None, :]
    cosine, sine = jnp.cos(angles), jnp.sin(angles)

    pair = prepare_pair(keys, values, cosine, sine)
    pair = lax.all_to_all(pair, ("yl", "sy"), split_axis=0, concat_axis=0, tiled=True)
    pair = pair.swapaxes(0, 1).reshape(2, 2, -1, width)
    block = pair.shape[2]
    own_values = pair[1].reshape(2, block // 128, 128, width).swapaxes(2, 3).reshape(2, block, width)
    c = jnp.concatenate([pair[0], own_values], axis=1)
    ahead = [(i, (i + 1) % 4) for i in range(4)]
    behind = [(i, (i - 1) % 4) for i in range(4)]
    swap = [(0, 1), (1, 0)]
    u = lax.ppermute(c, "x", ahead)
    v = lax.ppermute(c, "x", behind)
    near = []
    for piece in (c, u, v):
        near += [piece, lax.ppermute(piece, "core", swap)]
    far = []
    for source, half, way in ((near[2], 0, ahead), (near[4], 1, behind), (near[3], 0, ahead), (near[5], 1, behind)):
        far.append(lax.ppermute(source[half:half + 1], "x", way))
    pieces = near + [far[0], far[2], far[1], far[3]]
    where = jnp.stack([x, core]).astype(jnp.int32)

    ordered = prepare_queries(queries, cosine, sine, group)
    arrived = []
    for n in range(CHUNKS):
        arrived.append(lax.all_to_all(ordered[n], AXES, split_axis=0, concat_axis=0, tiled=True))
    halves = []
    for n in range(CHUNKS):
        done = attn(arrived[n], pieces, where, bq=TILE, period=rows, which=n)
        back = lax.all_to_all(done, AXES, split_axis=0, concat_axis=0, tiled=True)
        back = back.reshape(group, key_heads, -1, width).transpose(2, 1, 0, 3)
        halves.append(back.reshape(-1, heads_all, width))
    whole = lax.optimization_barrier(jnp.pad(halves[0], ((0, rows - rows // CHUNKS), (0, 0), (0, 0))))
    for n in range(1, CHUNKS):
        whole = lax.dynamic_update_slice(whole, halves[n], (n * (rows // CHUNKS), 0, 0))
    return whole


def solution(mesh):
    finer = Mesh(mesh.devices.reshape(4, 2, 2, 8), AXES)
    placed = P(AXES, None, None)

    return jax.shard_map(shards, mesh=finer, in_specs=(placed,) * 3, out_specs=placed, check_vma=False)
```
